8 devices in a mesh: batch: 1 (over z), w: 2 (over y), h: 4 (over x, core).
Axes of the slice: x: 2, y: 2, z: 1, core: 2. Of those that a mesh axis runs over, the one named last changes fastest.
Arguments:
- image: bfloat16 [128, 64, 512, 3], P('batch', 'h', 'w')
- down_w1: bfloat16 [3, 3, 3, 64], replicated
- down_v1: float32 [3, 64], replicated
- refine_w1: bfloat16 [3, 3, 64, 64], replicated
- refine_v1: float32 [3, 64], replicated
- down_w2: bfloat16 [3, 3, 64, 128], replicated
- down_v2: float32 [3, 128], replicated
- refine_w2: bfloat16 [3, 3, 128, 128], replicated
- refine_v2: float32 [3, 128], replicated
- down_w3: bfloat16 [3, 3, 128, 256], replicated
- down_v3: float32 [3, 256], replicated
- refine_w3: bfloat16 [3, 3, 256, 256], replicated
- refine_v3: float32 [3, 256], replicated
Outputs:
- output: bfloat16 [128, 8, 64, 256], P('batch', 'h', 'w')
All inputs are finite; a program needn't handle non-finite values.
Results may differ from the reference program's by a relative error of at most 0.00400014.
Values are sent between devices in bfloat16 or wider.
A program may use at most 1 GiB of HBM per device.

```python
import jax
import jax.numpy as jnp
from jax import lax

IMAGES = 128
IMG_HEIGHT = 64
IMG_WIDTH = 512
CHAN_IN = 3
CHAN_ONE = 64
GROUPS = 8
NORM_EPS = 1e-5


def draw_affine(key, channels):
    bias_key, scale_key, shift_key = jax.random.split(key, 3)
    bias = 0.5 * jax.random.normal(bias_key, (channels,), jnp.float32)
    scale = 1.0 + 0.3 * jax.random.normal(scale_key, (channels,), jnp.float32)
    shift = 0.3 * jax.random.normal(shift_key, (channels,), jnp.float32)
    return jnp.stack([bias, scale, shift])


def setup_inputs(seed: int = 0, part: int = 0) -> dict:
    shared_key, image_root = jax.random.split(jax.random.key(seed))
    image_key = jax.random.fold_in(image_root, part)
    noise_key, slope_key, level_key = jax.random.split(image_key, 3)
    noise = jax.random.normal(noise_key, (IMAGES, IMG_HEIGHT, IMG_WIDTH, CHAN_IN), jnp.float32)
    slopes = jax.random.normal(slope_key, (2, IMAGES, 1, 1, CHAN_IN), jnp.float32)
    levels = 0.5 * jax.random.normal(level_key, (IMAGES, 1, 1, CHAN_IN), jnp.float32)
    row_pos = (jnp.arange(IMG_HEIGHT, dtype=jnp.float32) + 0.5) * (2.0 / IMG_HEIGHT) - 1.0
    col_pos = (jnp.arange(IMG_WIDTH, dtype=jnp.float32) + 0.5) * (2.0 / IMG_WIDTH) - 1.0
    ramp = slopes[0] * row_pos[:, None, None] + slopes[1] * col_pos[:, None]
    image = (noise + 1.5 * ramp + levels).astype(jnp.bfloat16)
    widths = [CHAN_IN, CHAN_ONE, 2 * CHAN_ONE, 4 * CHAN_ONE]
    weight_keys = jax.random.split(shared_key, 12)
    inputs = {"image": image}
    for stage in range(3):
        chan_prev = widths[stage]
        chan_next = widths[stage + 1]
        down_w = jax.random.normal(weight_keys[4 * stage], (3, 3, chan_prev, chan_next), jnp.float32) * (9 * chan_prev) ** -0.5
        refine_w = jax.random.normal(weight_keys[4 * stage + 2], (3, 3, chan_next, chan_next), jnp.float32) * (9 * chan_next) ** -0.5
        inputs["down_w" + str(stage + 1)] = down_w.astype(jnp.bfloat16)
        inputs["down_v" + str(stage + 1)] = draw_affine(weight_keys[4 * stage + 1], chan_next)
        inputs["refine_w" + str(stage + 1)] = refine_w.astype(jnp.bfloat16)
        inputs["refine_v" + str(stage + 1)] = draw_affine(weight_keys[4 * stage + 3], chan_next)
    return inputs


def conv_norm(inputs, kernel, affine, stride):
    summed = lax.conv_general_dilated(inputs.astype(jnp.float32), kernel.astype(jnp.float32), (stride, stride), ((1, 1), (1, 1)), dimension_numbers=("NHWC", "HWIO", "NHWC")) + affine[0]
    out_shape = summed.shape
    grouped = summed.reshape(out_shape[0], out_shape[1], out_shape[2], GROUPS, out_shape[3] // GROUPS)
    grp_mean = jnp.mean(grouped, axis=(1, 2, 4), keepdims=True)
    centered = grouped - grp_mean
    grp_var = jnp.mean(jnp.square(centered), axis=(1, 2, 4), keepdims=True)
    normed = (centered * lax.rsqrt(grp_var + NORM_EPS)).reshape(out_shape)
    return jax.nn.relu(normed * affine[1] + affine[2]).astype(jnp.bfloat16)


def reference(image, down_w1, down_v1, refine_w1, refine_v1, down_w2, down_v2, refine_w2, refine_v2, down_w3, down_v3, refine_w3, refine_v3):
    stages = ((down_w1, down_v1, refine_w1, refine_v1), (down_w2, down_v2, refine_w2, refine_v2), (down_w3, down_v3, refine_w3, refine_v3))

    def one_image(single):
        current = single[None]
        for down_w, down_v, refine_w, refine_v in stages:
            current = conv_norm(current, down_w, down_v, 2)
            current = conv_norm(current, refine_w, refine_v, 1)
        return current[0]

    return lax.map(one_image, image)
```

```python
import jax
import jax.numpy as jnp
from jax import lax
from jax.experimental import pallas as pl
from jax.experimental.pallas import tpu as pltpu
from jax.sharding import PartitionSpec as P

NORM_EPS = 1e-5
BF = jnp.bfloat16
F32 = jnp.float32
PAIR, SUB, TILE, LANES, WIDE = 2, 8, 16, 128, 256
PEERS, GROUPS, HALVES = 8, 8, 2
C1, C2, C3 = 64, 128, 256
PHASES, PIECE_ROWS, PIECE_COLS = 5, 48, 256
AREAS = (32 * 256, 16 * 128, 8 * 64)
MESH = pl.DeviceIdType.MESH
LOW, HIGH = slice(None, LANES), slice(LANES, None)


def dot(lhs, rhs):
    return jnp.dot(lhs, rhs, preferred_element_type=F32)


def iota(shape, dim):
    return lax.broadcasted_iota(jnp.int32, shape, dim)


def one_hot(mask):
    return jnp.where(mask, 1.0, 0.0).astype(BF)


def join(parts, axis=0):
    return jnp.concatenate(parts, axis=axis)


def rows_of(ref, index, first, count):
    return ref[index, first:first + count].reshape(count * TILE, ref.shape[-1])


def tiles_of(block):
    return block.reshape(-1, TILE, WIDE)


def lane_half(ref, half):
    return ref.at[..., LOW] if half == 0 else ref.at[..., HIGH]


def expand_first(down1, taps, w1):
    taps[...] = jnp.zeros(taps.shape, F32)
    for dy in range(3):
        for dx in range(3):
            taps[pl.ds(9 * dy + 3 * dx, 3), :] = down1[dy, dx].astype(F32)
    source = taps[...].astype(BF)
    row, tap = iota((WIDE, 32), 0), iota((WIDE, 32), 1)
    colour_phase = (row % LANES) // SUB
    colour, phase = colour_phase // PHASES, colour_phase % PHASES
    line = SUB * (row // LANES) + row % SUB
    for o in range(HALVES):
        lanes = []
        for cp in range(HALVES):
            for rp in range(HALVES):
                dy, dx = line - 7 - 4 * o - 2 * rp, phase - 2 * cp
                inside = (dy >= 0) & (dy < 3) & (dx >= 0) & (dx < 3) & (colour < 3)
                lanes.append(dot(one_hot(inside & (tap == 9 * dy + 3 * dx + colour)), source))
        w1[o] = join(lanes, 1).astype(BF)


def expand_refine1(refine1, wr1):
    blank = jnp.zeros((C1, C1), BF)
    wr1[...] = jnp.zeros(wr1.shape, BF)
    for dx in range(3):
        for y in range(4):
            pair = join([refine1[y, dx] if y < 3 else blank, refine1[y - 1, dx] if y else blank], 1)
            for cp in range(HALVES):
                lane_half(wr1, cp)[pl.ds(((dx + cp) * 4 + y) * C1, C1), :] = pair


def expand_rows(kernel, out, shift, order):
    depth = kernel.shape[2]
    out[...] = jnp.zeros(out.shape, BF)
    for dy in range(3):
        for dx in range(3):
            for r in range(HALVES):
                lane_half(out, r)[pl.ds(order(dy + shift * r, dx) * depth, depth), :] = kernel[dy, dx]


def encoder_kernel(image, down1, v1, refine1, v2, down2, v3, refine2, v4, wd3, v5, wr3, v6, out, inbuf, outbuf, in_send, in_recv, out_send, out_recv, taps,
                   vecs, w1, wr1, wd2, wr2, perm, gmat, af, bs, abuf, y1e, y1o, z1e, z1o, y2, z2e, z2o, y3, obuf):
    group = pl.program_id(0)
    me = 2 * lax.axis_index("h") + lax.axis_index("w")

    def peer(k):
        return lax.rem(me + k, PEERS)

    def device(index):
        return {"h": index // 2, "w": lax.rem(index, 2)}

    def images(index, g):
        return pl.ds(index * PAIR * GROUPS + PAIR * g, PAIR)

    def send_in(g, to, sender):
        return pltpu.make_async_remote_copy(image.at[images(to, g)], inbuf.at[g, sender], in_send.at[g, to], in_recv.at[g, sender], device_id=device(to), device_id_type=MESH)

    def keep_in(g):
        return pltpu.make_async_copy(image.at[images(me, g)], inbuf.at[g, me], in_recv.at[g, me])

    def send_out(g, to, sender):
        return pltpu.make_async_remote_copy(outbuf.at[g, to], out.at[images(sender, g)], out_send.at[g, to], out_recv.at[g, sender], device_id=device(to), device_id_type=MESH)

    def keep_out(g):
        return pltpu.make_async_copy(outbuf.at[g, me], out.at[images(me, g)], out_recv.at[g, me])

    def start_out(g):
        for k in range(1, PEERS):
            send_out(g, peer(k), me).start()
        keep_out(g).start()

    @pl.when(group == 0)
    def _():
        barrier = pltpu.get_barrier_semaphore()
        for k in range(1, PEERS):
            pl.semaphore_signal(barrier, inc=1, device_id=device(peer(k)), device_id_type=MESH)
        pl.semaphore_wait(barrier, PEERS - 1)

        def begin(g, _):
            keep_in(g).start()
            for k in range(1, PEERS):
                send_in(g, peer(k), me).start()
            return 0

        lax.fori_loop(0, GROUPS, begin, 0)

        expand_first(down1, taps, w1)
        expand_refine1(refine1, wr1)
        expand_rows(down2, wd2, 2, lambda y, x: 6 * x + y)
        expand_rows(refine2, wr2, 1, lambda y, x: 3 * y + x)
        for i, ref in enumerate((v1, v2, v3, v4, v5, v6)):
            vecs[i] = join([ref[...]] * (WIDE // ref.shape[1]), 1)
        row, lane = iota((2 * WIDE, LANES), 0), iota((2 * WIDE, LANES), 1)
        for d in range(PHASES):
            perm[:, d * LANES:(d + 1) * LANES] = one_hot(row == 4 * ((lane % SUB) * TILE + lane // SUB) + d - 1)
        row, lane = iota((WIDE, WIDE), 0), iota((WIDE, WIDE), 1)
        for g, rep in enumerate((C1, C2, C3)):
            gmat[g] = one_hot((row % rep) // (rep // SUB) == (lane % rep) // (rep // SUB))
        for ref in (y1e, y1o, y2, y3, z2e, z2o, bs):
            ref[0] = jnp.zeros(ref.shape[1:], BF)
        for ref in (y1e, y1o, y2, y3):
            ref[ref.shape[0] - 1] = jnp.zeros(ref.shape[1:], BF)

    @pl.when(group > 0)
    def _():
        start_out(group - 1)

    keep_in(group).wait()
    for k in range(1, PEERS):
        send_in(group, peer(k), peer(k)).wait_recv()

    strip = iota((SUB, LANES), 0)
    not_first = jnp.where(strip == 0, 0.0, 1.0)
    not_last = jnp.where(strip == SUB - 1, 0.0, 1.0)

    def from_left(tile):
        return join([pltpu.roll(tile[SUB * e:SUB * e + SUB], 1, 0) * not_first for e in range(PAIR)]).astype(BF)

    def from_right(tile):
        return join([pltpu.roll(tile[SUB * e:SUB * e + SUB], SUB - 1, 0) * not_last for e in range(PAIR)]).astype(BF)

    def moments(acc, carry):
        tiles = tiles_of(acc)
        return carry[0] + jnp.sum(tiles, axis=0), carry[1] + jnp.sum(tiles * tiles, axis=0)

    def conv(trips, body):
        zeros = jnp.zeros((TILE, WIDE), F32)
        return lax.fori_loop(0, trips, body, (zeros, zeros))

    def finalize(layer, sums):
        rep = (C1, C2, C3)[layer // 2]
        area = AREAS[layer // 2]
        per_strip = area * rep / (WIDE * SUB)
        count = float(area * rep // SUB)
        bias, gain, offset = vecs[layer, 0:1, :], vecs[layer, 1:2, :], vecs[layer, 2:3, :]
        first = sums[0] + per_strip * bias
        second = sums[1] + 2.0 * bias * sums[0] + per_strip * bias * bias
        rest = join([first, second])
        parts = []
        for _ in range(3):
            parts.append(rest.astype(BF))
            rest = rest - parts[-1].astype(F32)
        grouped = jnp.sum(dot(join(parts), gmat[layer // 2]).reshape(3, 2 * PAIR, SUB, WIDE), axis=0)
        grouped = jnp.sum(grouped, axis=1, keepdims=True) / count
        scales, shifts = [], []
        for e in range(PAIR):
            mean, square = grouped[e], grouped[PAIR + e]
            scale = lax.rsqrt(jnp.maximum(square - mean * mean, 0.0) + NORM_EPS) * gain
            scales.append(jnp.broadcast_to(scale, (SUB, WIDE)))
            shifts.append(jnp.broadcast_to(offset + (bias - mean) * scale, (SUB, WIDE)))
        return join(scales), join(shifts)

    def apply(block, norm):
        return jnp.maximum(block * norm[0] + norm[1], 0.0)

    for e in range(PAIR):
        sides = [join([inbuf[group, HALVES * hh + half, e] for hh in range(4)]) for half in range(HALVES)]
        af[e] = dot(join(sides, 1), perm[...]).reshape(af.shape[1:])

    def im2col(k, _):
        pair = []
        for e in range(PAIR):
            rows = []
            for c in range(3):
                block = af[e, (k // 2) * 6 + c * 2 + lax.rem(k, 2)]
                rows += [block[:, d * LANES:(d + 1) * LANES] for d in range(PHASES)]
            rows.append(jnp.zeros((SUB, LANES), F32))
            pair.append(join(rows).T.reshape(TILE, SUB, LANES))
        bs[k + 1] = join(pair, 1).astype(BF)
        return 0

    lax.fori_loop(0, SUB, im2col, 0)

    def conv_down1(k, carry):
        lhs = join([rows_of(bs, k, 0, TILE), rows_of(bs, k + 1, 0, TILE)], 1)
        for o in range(HALVES):
            acc = dot(lhs, w1[o])
            abuf[2 * k + o] = tiles_of(acc)
            carry = moments(acc, carry)
        return carry

    norm = finalize(0, conv(SUB, conv_down1))

    def norm1(i, _):
        val = apply(abuf[i], norm)
        y1e[i + 1, 0:TILE] = val[..., LOW].astype(BF)
        y1o[i + 1, 1:] = val[..., HIGH].astype(BF)
        y1o[i + 1, 0] = from_left(val[TILE - 1][:, HIGH])
        y1e[i + 1, TILE] = from_right(val[0][:, LOW])
        return 0

    lax.fori_loop(0, TILE, norm1, 0)

    def refine1_lhs(rows):
        tiles = []
        for first in range(2):
            for ref in (y1o, y1e):
                for a in range(2):
                    tiles.append(join([rows_of(ref, i + a, first, TILE) for i in rows]))
        return join(tiles, 1)

    upper = (iota((1, WIDE), 1) % LANES) < C1
    keep = {0: jnp.where(upper, 0.0, 1.0), TILE: jnp.where(upper, 1.0, 0.0)}

    def conv_refine1(t, carry):
        rows = [1 + 3 * t + r for r in range(3)]
        acc = dot(refine1_lhs(rows), wr1[...])
        for r, i in enumerate(rows):
            abuf[i] = tiles_of(acc)[r * TILE:(r + 1) * TILE]
        return moments(acc, carry)

    carry = conv(5, conv_refine1)
    acc = dot(refine1_lhs(list(keep)), wr1[...])
    for part, i in enumerate(keep):
        edge = acc[part * WIDE:(part + 1) * WIDE] * keep[i]
        abuf[i] = tiles_of(edge)
        carry = moments(edge, carry)
    norm = finalize(1, carry)

    def norm2_row(i, val):
        z1e[i] = val[..., LOW].astype(BF)
        z1o[i, 1:] = val[..., HIGH].astype(BF)
        z1o[i, 0] = from_left(val[TILE - 1][:, HIGH])

    def norm2(i, _):
        norm2_row(i, apply(abuf[i], norm))
        return 0

    lax.fori_loop(1, TILE, norm2, 0)
    for i in keep:
        norm2_row(i, apply(abuf[i], norm) * keep[i])

    def put_pair(acc, t):
        half = acc.shape[0] // 2
        abuf[2 * t] = tiles_of(acc[:half])
        abuf[2 * t + 1] = tiles_of(acc[half:])

    def conv_down2(t, carry):
        tiles = []
        for ref, first in ((z1o, 0), (z1e, 0), (z1o, 1)):
            for a in range(3):
                tiles.append(join([rows_of(ref, 4 * t + 2 * u + a, first, TILE) for u in range(2)]))
        acc = dot(join(tiles, 1), wd2[...])
        put_pair(acc, t)
        return moments(acc, carry)

    norm = finalize(2, conv(4, conv_down2))

    def norm3(u, _):
        val = apply(abuf[u], norm)
        for v, part in enumerate((LOW, HIGH)):
            row = val[..., part]
            y2[2 * u + v + 1, 1:TILE + 1] = row.astype(BF)
            y2[2 * u + v + 1, 0] = from_left(row[TILE - 1])
            y2[2 * u + v + 1, TILE + 1] = from_right(row[0])
        return 0

    lax.fori_loop(0, SUB, norm3, 0)

    def conv_refine2(t, carry):
        tiles = []
        for a in range(4):
            for b in range(3):
                tiles.append(join([rows_of(y2, 4 * t + 2 * u + a, b, TILE) for u in range(2)]))
        acc = dot(join(tiles, 1), wr2[...])
        put_pair(acc, t)
        return moments(acc, carry)

    norm = finalize(3, conv(4, conv_refine2))

    def norm4(u, _):
        for q in range(TILE):
            val = apply(abuf[u, q], norm)
            for v, part in enumerate((LOW, HIGH)):
                if q % 2:
                    z2o[2 * u + v + 1, q // 2 + 1] = val[:, part].astype(BF)
                else:
                    z2e[2 * u + v + 1, q // 2] = val[:, part].astype(BF)
                if q == TILE - 1:
                    z2o[2 * u + v + 1, 0] = from_left(val[:, part])
        return 0

    lax.fori_loop(0, SUB, norm4, 0)

    def conv_down3(t, carry):
        tiles = []
        for a in range(3):
            for ref, first in ((z2o, 0), (z2e, 0), (z2o, 1)):
                tiles.append(join([rows_of(ref, 8 * t + 2 * p + a, first, SUB) for p in range(4)]))
        acc = dot(join(tiles, 1), wd3[...])
        put_pair(acc, t)
        return moments(acc, carry)

    norm = finalize(4, conv(2, conv_down3))

    def norm5(u, _):
        val = apply(abuf[u], norm)
        for v in range(2):
            row = val[SUB * v:SUB * v + SUB]
            y3[2 * u + v + 1, 1:SUB + 1] = row.astype(BF)
            y3[2 * u + v + 1, 0] = join([from_left(row[SUB - 1][:, part]) for part in (LOW, HIGH)], 1)
            y3[2 * u + v + 1, SUB + 1] = join([from_right(row[0][:, part]) for part in (LOW, HIGH)], 1)
        return 0

    lax.fori_loop(0, 4, norm5, 0)

    def conv_refine3(t, carry):
        tiles = []
        for a in range(3):
            for b in range(3):
                tiles.append(join([rows_of(y3, 4 * t + p + a, b, SUB) for p in range(4)]))
        acc = dot(join(tiles, 1), wr3[...])
        put_pair(acc, t)
        return moments(acc, carry)

    norm = finalize(5, conv(2, conv_refine3))

    def norm6(u, _):
        val = apply(abuf[u], norm)
        for v in range(2):
            for e in range(PAIR):
                for h, part in enumerate((LOW, HIGH)):
                    for q in range(SUB):
                        obuf[v, e, h, pl.ds(q, SUB, SUB), :] = val[SUB * v + q, SUB * e:SUB * e + SUB, part]
                    for w in range(HALVES):
                        outbuf[group, 2 * u + w, e, v, :, part] = obuf[v, e, h, 32 * w:32 * w + 32].astype(BF)
        return 0

    lax.fori_loop(0, 4, norm6, 0)

    @pl.when(group == GROUPS - 1)
    def _():
        def sent(g, _):
            for k in range(1, PEERS):
                send_in(g, peer(k), me).wait_send()
            return 0

        lax.fori_loop(0, GROUPS, sent, 0)
        start_out(group)

        def done(g, _):
            for k in range(1, PEERS):
                send_out(g, peer(k), me).wait_send()
                send_out(g, peer(k), peer(k)).wait_recv()
            keep_out(g).wait()
            return 0

        lax.fori_loop(0, GROUPS, done, 0)


def solution(mesh):
    act_spec = P("batch", "h", "w")
    sems = pltpu.SemaphoreType.DMA((GROUPS, PEERS))
    scratch = [
        ((GROUPS, PEERS, PAIR, PIECE_ROWS, PIECE_COLS), BF), ((GROUPS, PEERS, PAIR, 2, 32, WIDE), BF), None, None, None, None, ((32, C1), F32),
        ((6, 3, WIDE), F32), ((2, WIDE, WIDE), BF), ((1024, WIDE), BF), ((1152, WIDE), BF), ((1536, WIDE), BF), ((512, 640), BF), ((3, WIDE, WIDE), BF),
        ((PAIR, 24, SUB, 640), F32), ((9, TILE, TILE, LANES), BF), ((17, TILE, TILE, WIDE), F32),
        ((18, 17, TILE, LANES), BF), ((18, 17, TILE, LANES), BF), ((17, 16, TILE, LANES), BF), ((17, 17, TILE, LANES), BF),
        ((18, 18, TILE, LANES), BF), ((17, 8, TILE, LANES), BF), ((17, 9, TILE, LANES), BF), ((10, 10, TILE, WIDE), BF), ((2, PAIR, 2, 64, LANES), F32),
    ]

    def local_forward(tile, *params):
        planes = tile.transpose(0, 3, 1, 2).reshape(-1, PIECE_ROWS, PIECE_COLS)
        params = list(params)
        params[8], params[10] = params[8].reshape(-1, WIDE), params[10].reshape(-1, WIDE)
        return pl.pallas_call(
            encoder_kernel,
            grid=(GROUPS,),
            out_shape=jax.ShapeDtypeStruct((128, 2, 32, WIDE), BF),
            in_specs=[pl.BlockSpec(memory_space=pl.ANY)] + [pl.BlockSpec(memory_space=pltpu.VMEM)] * 12,
            out_specs=pl.BlockSpec(memory_space=pl.ANY),
            scratch_shapes=[sems if entry is None else pltpu.VMEM(*entry) for entry in scratch],
            compiler_params=pltpu.CompilerParams(vmem_limit_bytes=60 * 1024 * 1024, collective_id=0, has_side_effects=True),
            name="encoder",
        )(planes, *params)

    return jax.shard_map(local_forward, mesh=mesh, in_specs=(act_spec,) + (P(),) * 12, out_specs=act_spec, check_vma=False)
```

```python
import jax
import jax.numpy as jnp
from jax import lax
from jax.experimental import pallas as pl
from jax.experimental.pallas import tpu as pltpu
from jax.sharding import PartitionSpec as P

NORM_EPS = 1e-5
BF = jnp.bfloat16
F32 = jnp.float32
PAIR, SUB, TILE, LANES, WIDE, UNIT = 2, 8, 16, 128, 256, 128
CHUNK = 4
PEERS, GROUPS, HALVES = 8, 8, 2
C1, C2, C3 = 64, 128, 256
PHASES, PIECE_ROWS, PIECE_COLS = 5, 48, 256
AREAS = (32 * 256, 16 * 128, 8 * 64)
MESH = pl.DeviceIdType.MESH
LOW, HIGH = slice(None, LANES), slice(LANES, None)


def iota(shape, dim):
    return lax.broadcasted_iota(jnp.int32, shape, dim)


def one_hot(mask):
    return jnp.where(mask, 1.0, 0.0).astype(BF)


def join(parts, axis=0):
    return jnp.concatenate(parts, axis=axis)


def side_by_side(parts):
    return jnp.concatenate(parts, axis=1)


def rows_of(ref, index, first, count):
    return ref[index, first:first + count].reshape(count * TILE, ref.shape[-1])


def dot(lhs, rhs):
    return jnp.dot(lhs, rhs, preferred_element_type=F32)


def lane_half(ref, half):
    return ref.at[..., LOW] if half == 0 else ref.at[..., HIGH]


def expand_first(down1, taps, w1):
    taps[...] = jnp.zeros(taps.shape, F32)
    for dy in range(3):
        for dx in range(3):
            taps[pl.ds(9 * dy + 3 * dx, 3), :] = down1[dy, dx].astype(F32)
    source = taps[...].astype(BF)
    row, tap = iota((WIDE, 32), 0), iota((WIDE, 32), 1)
    colour_phase = (row % LANES) // SUB
    colour, phase = colour_phase // PHASES, colour_phase % PHASES
    line = SUB * (row // LANES) + row % SUB
    for o in range(HALVES):
        lanes = []
        for cp in range(HALVES):
            for rp in range(HALVES):
                dy, dx = line - 7 - 4 * o - 2 * rp, phase - 2 * cp
                inside = (dy >= 0) & (dy < 3) & (dx >= 0) & (dx < 3) & (colour < 3)
                lanes.append(dot(one_hot(inside & (tap == 9 * dy + 3 * dx + colour)), source))
        w1[:, o * WIDE:(o + 1) * WIDE] = side_by_side(lanes).astype(BF)


def expand_refine1(refine1, wr1):
    blank = jnp.zeros((C1, C1), BF)
    wr1[...] = jnp.zeros(wr1.shape, BF)
    for dx in range(3):
        for y in range(4):
            pair = side_by_side([refine1[y, dx] if y < 3 else blank, refine1[y - 1, dx] if y else blank])
            for cp in range(HALVES):
                lane_half(wr1, cp)[pl.ds(((y // 2 * 4 + dx + cp) * 2 + y % 2) * C1, C1), :] = pair


def expand_rows(kernel, out, shift, order):
    depth = kernel.shape[2]
    out[...] = jnp.zeros(out.shape, BF)
    for dy in range(3):
        for dx in range(3):
            for r in range(HALVES):
                lane_half(out, r)[pl.ds(order(dy + shift * r, dx) * depth, depth), :] = kernel[dy, dx]


def from_left(tile, strip):
    return jnp.where(strip == 0, 0.0, pltpu.roll(tile, 1, 0)).astype(BF)


def from_right(tile, strip):
    return jnp.where(strip == TILE - 1, 0.0, pltpu.roll(tile, TILE - 1, 0)).astype(BF)


class Stream:
    def __init__(self, params, buffers, put):
        self.put = put
        self.vecs, self.gmat, self.w1, self.wr1, self.wd2, self.wr2, self.wd3, self.wr3 = params
        self.bs, self.abuf, self.y1e, self.y1o, self.z1e, self.z1o, self.y2, self.z2e, self.z2o, self.y3, self.obuf, self.sums, self.norm = buffers
        self.strip = iota((TILE, LANES), 0)
        upper = (iota((1, WIDE), 1) % LANES) < C1
        self.keep = {0: jnp.where(upper, 0.0, 1.0), TILE: jnp.where(upper, 1.0, 0.0)}


    def lhs0(self, unit, step):
        return side_by_side([rows_of(self.bs, unit + n, 0, SUB) for n in range(2)])

    def lhs1(self, unit, step):
        return side_by_side([rows_of(ref, unit + step // 2, step % 2, SUB) for ref in (self.y1o, self.y1e)])

    def ninth(self, tile, step):
        return side_by_side([tile(2 * step), tile(2 * step + 1)]) if step < 4 else tile(2 * step)

    def lhs2(self, unit, step):
        taps = ((self.z1o, 0), (self.z1e, 0), (self.z1o, 1))

        def tile(n):
            ref, first = taps[n // 3]
            return rows_of(ref, 2 * unit + n % 3, first, SUB)

        return self.ninth(tile, step)

    def lhs3(self, unit, step):
        return side_by_side([rows_of(self.y2, 2 * unit + n // 3, n % 3, SUB) for n in (2 * step, 2 * step + 1)])

    def lhs4(self, unit, step):
        taps = ((self.z2o, 0), (self.z2e, 0), (self.z2o, 1))

        def tile(n):
            ref, first = taps[n % 3]
            return join([rows_of(ref, 2 * (2 * unit + p) + n // 3, first, 4) for p in range(2)])

        return self.ninth(tile, step)

    def lhs5(self, unit, step):
        return join([rows_of(self.y3, 2 * unit + p + step // 3, step % 3, 4) for p in range(2)])

    def finish(self, layer, unit, val):
        if layer == 1 and unit in self.keep:
            val = val * self.keep[unit]
        tiles = val.reshape(SUB, TILE, WIDE)
        self.abuf[unit] = tiles
        self.total[0] += jnp.sum(tiles, axis=0)
        self.total[1] += jnp.sum(tiles * tiles, axis=0)

    def conv(self, layer):
        lhs = (self.lhs0, self.lhs1, self.lhs2, self.lhs3, self.lhs4, self.lhs5)[layer]
        steps, ref, count = ((1, self.w1, SUB), (4, self.wr1, 15), (5, self.wd2, SUB), (6, self.wr2, SUB), (5, self.wd3, 4), (9, self.wr3, 4))[layer]
        base = 1 if layer == 1 else 0

        def emit(units, first, last):
            rows = side_by_side([join([lhs(unit, step) for unit in units]) for step in range(first, last)])
            acc = dot(rows, ref[first * WIDE:first * WIDE + rows.shape[1], :])
            for n, unit in enumerate(units):
                part = acc[n * UNIT:(n + 1) * UNIT]
                if layer == 0:
                    self.finish(layer, 2 * unit, part[:, :WIDE])
                    self.finish(layer, 2 * unit + 1, part[:, WIDE:])
                else:
                    self.finish(layer, unit, part)

        def chunk(c):
            emit([base + n for n in range(CHUNK * c, min(CHUNK * (c + 1), count))], 0, steps)

        items = [lambda c=c: chunk(c) for c in range(-(-count // CHUNK))]
        if layer == 1:
            items.append(lambda: (emit([0], 2, 4), emit([TILE], 0, 2)))

        def start():
            self.total = [jnp.zeros((TILE, WIDE), F32)] * 2

        def store():
            for n in range(2):
                self.sums[n] = self.total[n]

        return [start, *items, store]

    def finalize(self, layer):
        rep = (C1, C2, C3)[layer // 2]
        area = AREAS[layer // 2]
        per_strip = area * rep / (WIDE * SUB)
        count = float(area * rep // SUB)
        bias, gain, offset = self.vecs[layer, 0:1, :], self.vecs[layer, 1:2, :], self.vecs[layer, 2:3, :]
        plain, square = [self.sums[n, :SUB] + self.sums[n, SUB:] for n in range(2)]
        rest = join([plain + per_strip * bias, square + 2.0 * bias * plain + per_strip * bias * bias])
        parts = []
        for _ in range(3):
            parts.append(rest.astype(BF))
            rest = rest - parts[-1].astype(F32)
        grouped = dot(join(parts), self.gmat[layer // 2])
        grouped = grouped[:TILE] + grouped[TILE:2 * TILE] + grouped[2 * TILE:]
        mean = jnp.sum(grouped[:SUB], axis=0, keepdims=True) / count
        power = jnp.sum(grouped[SUB:], axis=0, keepdims=True) / count
        scale = lax.rsqrt(jnp.maximum(power - mean * mean, 0.0) + NORM_EPS) * gain
        self.affine = [jnp.broadcast_to(row, (TILE, WIDE)) for row in (scale, offset + (bias - mean) * scale)]

    def apply(self, block):
        return jnp.maximum(block * self.affine[0] + self.affine[1], 0.0)

    def row0(self, i):
        val = self.apply(self.abuf[i])
        self.y1e[i + 1, 0:SUB] = val[..., LOW].astype(BF)
        self.y1o[i + 1, 1:] = val[..., HIGH].astype(BF)
        self.y1o[i + 1, 0] = from_left(val[SUB - 1][:, HIGH], self.strip)
        self.y1e[i + 1, SUB] = from_right(val[0][:, LOW], self.strip)

    def row1(self, i):
        val = self.apply(self.abuf[i])
        if i in self.keep:
            val = val * self.keep[i]
        self.z1e[i] = val[..., LOW].astype(BF)
        self.z1o[i, 1:] = val[..., HIGH].astype(BF)
        self.z1o[i, 0] = from_left(val[SUB - 1][:, HIGH], self.strip)

    def row2(self, u):
        val = self.apply(self.abuf[u])
        for v, part in enumerate((LOW, HIGH)):
            line = val[..., part]
            self.y2[2 * u + v + 1, 1:SUB + 1] = line.astype(BF)
            self.y2[2 * u + v + 1, 0] = from_left(line[SUB - 1], self.strip)
            self.y2[2 * u + v + 1, SUB + 1] = from_right(line[0], self.strip)

    def row3(self, u):
        val = self.apply(self.abuf[u])
        for v, part in enumerate((LOW, HIGH)):
            for q in range(SUB):
                pixel = val[q][:, part]
                if q % 2:
                    self.z2o[2 * u + v + 1, q // 2 + 1] = pixel.astype(BF)
                else:
                    self.z2e[2 * u + v + 1, q // 2] = pixel.astype(BF)
            self.z2o[2 * u + v + 1, 0] = from_left(val[SUB - 1][:, part], self.strip)

    def row4(self, u):
        val = self.apply(self.abuf[u])
        for v in range(2):
            line = val[4 * v:4 * v + 4]
            self.y3[2 * u + v + 1, 1:5] = line.astype(BF)
            self.y3[2 * u + v + 1, 0] = side_by_side([from_left(line[3][:, part], self.strip) for part in (LOW, HIGH)])
            self.y3[2 * u + v + 1, 5] = side_by_side([from_right(line[0][:, part], self.strip) for part in (LOW, HIGH)])

    def row5(self, u):
        val = self.apply(self.abuf[u])
        for v in range(2):
            for h, part in enumerate((LOW, HIGH)):
                for q in range(4):
                    self.obuf[u, v, h, pl.ds(q, TILE, 4), :] = val[4 * v + q][:, part]
                for w in range(HALVES):
                    self.put(2 * u + w, v, part, self.obuf[u, v, h, 32 * w:32 * w + 32].astype(BF))

    def post(self, layer):
        row, count = ((self.row0, TILE), (self.row1, TILE + 1), (self.row2, SUB), (self.row3, SUB), (self.row4, 4), (self.row5, 4))[layer]
        return [lambda: self.finalize(layer)] + [lambda i=i: row(i) for i in range(count)]


def blend(chunks, rest):
    done = 0
    for n, emit in enumerate(chunks):
        emit()
        goal = len(rest) * (n + 1) // len(chunks)
        for item in rest[done:goal]:
            item()
        done = goal
    for item in rest[done:]:
        item()


def encoder_kernel(image, down1, v1, refine1, v2, down2, v3, refine2, v4, wd3, v5, wr3, v6, out, inbuf, outbuf, in_send, in_recv, out_send, out_recv, taps,
                   vecs, w1, wr1, wd2, wr2, perm, gmat, af, *buffers):
    group = pl.program_id(0)
    me = 2 * lax.axis_index("h") + lax.axis_index("w")

    def peer(k):
        return lax.rem(me + k, PEERS)

    def device(index):
        return {"h": index // 2, "w": lax.rem(index, 2)}

    def images(index, g):
        return pl.ds(index * PAIR * GROUPS + PAIR * g, PAIR)

    def send_in(g, to, sender):
        return pltpu.make_async_remote_copy(image.at[images(to, g)], inbuf.at[g, sender], in_send.at[g, to], in_recv.at[g, sender], device_id=device(to), device_id_type=MESH)

    def keep_in(g):
        return pltpu.make_async_copy(image.at[images(me, g)], inbuf.at[g, me], in_recv.at[g, me])

    def send_out(g, to, sender):
        return pltpu.make_async_remote_copy(outbuf.at[g, to], out.at[images(sender, g)], out_send.at[g, to], out_recv.at[g, sender], device_id=device(to), device_id_type=MESH)

    def keep_out(g):
        return pltpu.make_async_copy(outbuf.at[g, me], out.at[images(me, g)], out_recv.at[g, me])

    def start_out(g):
        for k in range(1, PEERS):
            send_out(g, peer(k), me).start()
        keep_out(g).start()

    @pl.when(group == 0)
    def _():
        barrier = pltpu.get_barrier_semaphore()
        for k in range(1, PEERS):
            pl.semaphore_signal(barrier, inc=1, device_id=device(peer(k)), device_id_type=MESH)
        pl.semaphore_wait(barrier, PEERS - 1)

        def begin(g, _):
            keep_in(g).start()
            for k in range(1, PEERS):
                send_in(g, peer(k), me).start()
            return 0

        lax.fori_loop(0, GROUPS, begin, 0)

        expand_first(down1, taps, w1)
        expand_refine1(refine1, wr1)
        expand_rows(down2, wd2, 2, lambda y, x: 6 * x + y)
        expand_rows(refine2, wr2, 1, lambda y, x: 3 * y + x)
        for i, ref in enumerate((v1, v2, v3, v4, v5, v6)):
            vecs[i] = side_by_side([ref[...]] * (WIDE // ref.shape[1]))
        row, lane = iota((2 * WIDE, LANES), 0), iota((2 * WIDE, LANES), 1)
        for d in range(PHASES):
            perm[:, d * LANES:(d + 1) * LANES] = one_hot(row == 4 * ((lane % TILE) * SUB + lane // TILE) + d - 1)
        row, lane = iota((WIDE, WIDE), 0), iota((WIDE, WIDE), 1)
        for g, rep in enumerate((C1, C2, C3)):
            gmat[g] = one_hot((row % rep) // (rep // SUB) == (lane % rep) // (rep // SUB))
        for e in range(PAIR):
            bs, _, y1e, y1o, _, _, y2, z2e, z2o, y3 = buffers[e:10 * PAIR:PAIR]
            for ref in (y1e, y1o, y2, y3, z2e, z2o, bs):
                ref[0] = jnp.zeros(ref.shape[1:], BF)
            for ref in (y1e, y1o, y2, y3):
                ref[ref.shape[0] - 1] = jnp.zeros(ref.shape[1:], BF)

    @pl.when(group > 0)
    def _():
        start_out(group - 1)

    keep_in(group).wait()
    for k in range(1, PEERS):
        send_in(group, peer(k), peer(k)).wait_recv()

    def put_of(e):
        def put(to, v, part, val):
            outbuf[group, to, e, v, :, part] = val

        return put

    params = (vecs, gmat, w1, wr1, wd2, wr2, wd3, wr3)
    streams = [Stream(params, buffers[e::PAIR], put_of(e)) for e in range(PAIR)]

    sides = [join([inbuf[group, HALVES * hh + half, e] for e in range(PAIR) for hh in range(4)]) for half in range(HALVES)]
    af[...] = dot(side_by_side(sides), perm[...]).reshape(af.shape)

    def im2col(e, k):
        rows = []
        for c in range(3):
            block = 24 * e + (k // 2) * 6 + c * 2 + k % 2
            rows += [af[block, :, d * LANES:(d + 1) * LANES] for d in range(PHASES)]
        rows.append(jnp.zeros((SUB, LANES), F32))
        streams[e].bs[k + 1] = join(rows).T.astype(BF).reshape(SUB, TILE, LANES)

    def phase(chunks, rest):
        pl.when(group >= 0)(lambda: blend(chunks, rest))

    gather = [[lambda e=e, k=k: im2col(e, k) for k in range(SUB)] for e in range(PAIR)]
    first, second = streams
    phase([], gather[0])
    phase(first.conv(0), gather[1])
    for layer in range(6):
        phase(second.conv(layer), first.post(layer))
        phase(first.conv(layer + 1) if layer < 5 else [], second.post(layer))

    @pl.when(group == GROUPS - 1)
    def _():
        def sent(g, _):
            for k in range(1, PEERS):
                send_in(g, peer(k), me).wait_send()
            return 0

        lax.fori_loop(0, GROUPS, sent, 0)
        start_out(group)

        def done(g, _):
            for k in range(1, PEERS):
                send_out(g, peer(k), me).wait_send()
                send_out(g, peer(k), peer(k)).wait_recv()
            keep_out(g).wait()
            return 0

        lax.fori_loop(0, GROUPS, done, 0)


def solution(mesh):
    act_spec = P("batch", "h", "w")
    sems = pltpu.SemaphoreType.DMA((GROUPS, PEERS))
    scratch = [
        ((GROUPS, PEERS, PAIR, PIECE_ROWS, PIECE_COLS), BF), ((GROUPS, PEERS, PAIR, 2, 32, WIDE), BF), None, None, None, None, ((32, C1), F32),
        ((6, 3, WIDE), F32), ((WIDE, 512), BF), ((1024, WIDE), BF), ((1152, WIDE), BF), ((1536, WIDE), BF),
        ((512, 640), BF), ((3, WIDE, WIDE), BF), ((48, SUB, 640), F32),
    ]
    for shape, dtype in (
        ((9, SUB, TILE, LANES), BF), ((17, SUB, TILE, WIDE), F32), ((18, 9, TILE, LANES), BF), ((18, 9, TILE, LANES), BF), ((17, 8, TILE, LANES), BF),
        ((17, 9, TILE, LANES), BF), ((18, 10, TILE, LANES), BF), ((17, 4, TILE, LANES), BF), ((17, 5, TILE, LANES), BF), ((10, 6, TILE, WIDE), BF),
        ((4, 2, 2, 64, LANES), F32), ((2, TILE, WIDE), F32), ((2, TILE, WIDE), F32),
    ):
        scratch += [(shape, dtype)] * PAIR

    def local_forward(tile, *params):
        planes = tile.transpose(0, 3, 1, 2).reshape(-1, PIECE_ROWS, PIECE_COLS)
        params = list(params)
        params[8], params[10] = params[8].reshape(-1, WIDE), params[10].reshape(-1, WIDE)
        return pl.pallas_call(
            encoder_kernel,
            grid=(GROUPS,),
            out_shape=jax.ShapeDtypeStruct((128, 2, 32, WIDE), BF),
            in_specs=[pl.BlockSpec(memory_space=pl.ANY)] + [pl.BlockSpec(memory_space=pltpu.VMEM)] * 12,
            out_specs=pl.BlockSpec(memory_space=pl.ANY),
            scratch_shapes=[sems if entry is None else pltpu.VMEM(*entry) for entry in scratch],
            compiler_params=pltpu.CompilerParams(vmem_limit_bytes=60 * 1024 * 1024, collective_id=0, has_side_effects=True),
            name="encoder",
        )(planes, *params)

    return jax.shard_map(local_forward, mesh=mesh, in_specs=(act_spec,) + (P(),) * 12, out_specs=act_spec, check_vma=False)
```

```python
import jax
import jax.numpy as jnp
from jax import lax
from jax.experimental import pallas as pl
from jax.experimental.pallas import tpu as pltpu
from jax.sharding import PartitionSpec as P

NORM_EPS = 1e-5
BF = jnp.bfloat16
F32 = jnp.float32
PAIR, SUB, TILE, LANES, WIDE, UNIT = 2, 8, 16, 128, 256, 128
CHUNK = 2
PEERS, GROUPS, HALVES = 8, 8, 2
C1, C2, C3 = 64, 128, 256
PHASES, PIECE_ROWS, PIECE_COLS = 5, 48, 256
AREAS = (32 * 256, 16 * 128, 8 * 64)
MESH = pl.DeviceIdType.MESH
LOW, HIGH = slice(None, LANES), slice(LANES, None)


def iota(shape, dim):
    return lax.broadcasted_iota(jnp.int32, shape, dim)


def one_hot(mask):
    return jnp.where(mask, 1.0, 0.0).astype(BF)


def join(parts, axis=0):
    return jnp.concatenate(parts, axis=axis)


def side_by_side(parts):
    return jnp.concatenate(parts, axis=1)


def rows_of(ref, index, first, count):
    return ref[index, first:first + count].reshape(count * TILE, ref.shape[-1])


def dot(lhs, rhs):
    return jnp.dot(lhs, rhs, preferred_element_type=F32)


def lane_half(ref, half):
    return ref.at[..., LOW] if half == 0 else ref.at[..., HIGH]


def expand_first(down1, taps, w1):
    taps[...] = jnp.zeros(taps.shape, F32)
    for dy in range(3):
        for dx in range(3):
            taps[pl.ds(9 * dy + 3 * dx, 3), :] = down1[dy, dx].astype(F32)
    source = taps[...].astype(BF)
    row, tap = iota((WIDE, 32), 0), iota((WIDE, 32), 1)
    colour_phase = (row % LANES) // SUB
    colour, phase = colour_phase // PHASES, colour_phase % PHASES
    line = SUB * (row // LANES) + row % SUB
    for o in range(HALVES):
        lanes = []
        for cp in range(HALVES):
            for rp in range(HALVES):
                dy, dx = line - 7 - 4 * o - 2 * rp, phase - 2 * cp
                inside = (dy >= 0) & (dy < 3) & (dx >= 0) & (dx < 3) & (colour < 3)
                lanes.append(dot(one_hot(inside & (tap == 9 * dy + 3 * dx + colour)), source))
        w1[:, o * WIDE:(o + 1) * WIDE] = side_by_side(lanes).astype(BF)


def expand_refine1(refine1, wr1):
    blank = jnp.zeros((C1, C1), BF)
    wr1[...] = jnp.zeros(wr1.shape, BF)
    for dx in range(3):
        for y in range(4):
            pair = side_by_side([refine1[y, dx] if y < 3 else blank, refine1[y - 1, dx] if y else blank])
            for cp in range(HALVES):
                lane_half(wr1, cp)[pl.ds(((y // 2 * 4 + dx + cp) * 2 + y % 2) * C1, C1), :] = pair


def expand_rows(kernel, out, shift, order):
    depth = kernel.shape[2]
    out[...] = jnp.zeros(out.shape, BF)
    for dy in range(3):
        for dx in range(3):
            for r in range(HALVES):
                lane_half(out, r)[pl.ds(order(dy + shift * r, dx) * depth, depth), :] = kernel[dy, dx]


def from_left(tile, strip):
    return jnp.where(strip == 0, 0.0, pltpu.roll(tile, 1, 0)).astype(BF)


def from_right(tile, strip):
    return jnp.where(strip == TILE - 1, 0.0, pltpu.roll(tile, TILE - 1, 0)).astype(BF)


class Stream:
    def __init__(self, params, buffers, put):
        self.put = put
        self.zero, self.vecs, self.gmat, self.w1, self.wr1, self.wd2, self.wr2, self.wd3, self.wr3 = params
        self.bs, self.abuf, self.y1e, self.y1o, self.z1e, self.z1o, self.y2, self.z2e, self.z2o, self.y3, self.obuf, self.sums, self.norm = buffers
        self.strip = iota((TILE, LANES), 0)
        upper = (iota((1, WIDE), 1) % LANES) < C1
        self.keep = {0: jnp.where(upper, 0.0, 1.0), TILE: jnp.where(upper, 1.0, 0.0)}


    def lhs0(self, unit, step):
        return side_by_side([rows_of(self.bs, unit + n, 0, SUB) for n in range(2)])

    def lhs1(self, unit, step):
        return side_by_side([rows_of(ref, unit + step // 2, step % 2, SUB) for ref in (self.y1o, self.y1e)])

    def ninth(self, tile, step):
        return side_by_side([tile(2 * step), tile(2 * step + 1)]) if step < 4 else tile(2 * step)

    def lhs2(self, unit, step):
        taps = ((self.z1o, 0), (self.z1e, 0), (self.z1o, 1))

        def tile(n):
            ref, first = taps[n // 3]
            return rows_of(ref, 2 * unit + n % 3, first, SUB)

        return self.ninth(tile, step)

    def lhs3(self, unit, step):
        return side_by_side([rows_of(self.y2, 2 * unit + n // 3, n % 3, SUB) for n in (2 * step, 2 * step + 1)])

    def lhs4(self, unit, step):
        taps = ((self.z2o, 0), (self.z2e, 0), (self.z2o, 1))

        def tile(n):
            ref, first = taps[n % 3]
            return join([rows_of(ref, 2 * (2 * unit + p) + n // 3, first, 4) for p in range(2)])

        return self.ninth(tile, step)

    def lhs5(self, unit, step):
        return join([rows_of(self.y3, 2 * unit + p + step // 3, step % 3, 4) for p in range(2)])

    def finish(self, layer, unit, val):
        if layer == 1 and unit in self.keep:
            val = val * self.keep[unit]
        tiles = val.reshape(SUB, TILE, WIDE)
        self.abuf[unit] = tiles
        self.total[0] += jnp.sum(tiles, axis=0)
        self.total[1] += jnp.sum(tiles * tiles, axis=0)

    def conv(self, layer):
        lhs = (self.lhs0, self.lhs1, self.lhs2, self.lhs3, self.lhs4, self.lhs5)[layer]
        steps, ref, count = ((1, self.w1, SUB), (4, self.wr1, 15), (5, self.wd2, SUB), (6, self.wr2, SUB), (5, self.wd3, 4), (9, self.wr3, 4))[layer]
        base = 1 if layer == 1 else 0

        waiting = []

        def drain():
            while waiting:
                units, acc = waiting.pop(0)
                for n, unit in enumerate(units):
                    part = acc[n * UNIT:(n + 1) * UNIT]
                    if layer == 0:
                        self.finish(layer, 2 * unit, part[:, :WIDE])
                        self.finish(layer, 2 * unit + 1, part[:, WIDE:])
                    else:
                        self.finish(layer, unit, part)

        def emit(units, first, last):
            rows = side_by_side([join([lhs(unit, step) for unit in units]) for step in range(first, last)])
            acc = dot(rows, ref[first * WIDE:first * WIDE + rows.shape[1], :])
            drain()
            waiting.append((units, acc))

        def chunk(c):
            emit([base + n for n in range(CHUNK * c, min(CHUNK * (c + 1), count))], 0, steps)

        items = [lambda c=c: chunk(c) for c in range(-(-count // CHUNK))]
        if layer == 1:
            items.append(lambda: emit([0], 2, 4))
            items.append(lambda: emit([TILE], 0, 2))

        def start():
            self.total = [jnp.zeros((TILE, WIDE), F32)] * 2

        def store():
            drain()
            for n in range(2):
                self.sums[n] = self.total[n]

        return [start, *items, store]

    def finalize(self, layer):
        rep = (C1, C2, C3)[layer // 2]
        area = AREAS[layer // 2]
        per_strip = area * rep / (WIDE * SUB)
        count = float(area * rep // SUB)
        bias, gain, offset = self.vecs[layer, 0:1, :], self.vecs[layer, 1:2, :], self.vecs[layer, 2:3, :]
        plain, square = [self.sums[n, :SUB] + self.sums[n, SUB:] for n in range(2)]
        rest = join([plain + per_strip * bias, square + 2.0 * bias * plain + per_strip * bias * bias])
        parts = []
        for _ in range(3):
            parts.append(rest.astype(BF))
            rest = rest - parts[-1].astype(F32)
        grouped = dot(join(parts), self.gmat[layer // 2])
        grouped = grouped[:TILE] + grouped[TILE:2 * TILE] + grouped[2 * TILE:]
        mean = jnp.sum(grouped[:SUB], axis=0, keepdims=True) / count
        power = jnp.sum(grouped[SUB:], axis=0, keepdims=True) / count
        scale = lax.rsqrt(jnp.maximum(power - mean * mean, 0.0) + NORM_EPS) * gain
        self.affine = [jnp.broadcast_to(row, (TILE, WIDE)) for row in (scale, offset + (bias - mean) * scale)]

    def apply(self, block):
        return jnp.maximum(block * self.affine[0] + self.affine[1], 0.0)

    def row0(self, i):
        val = self.apply(self.abuf[self.zero + i])
        self.y1e[i + 1, 0:SUB] = val[..., LOW].astype(BF)
        self.y1o[i + 1, 1:] = val[..., HIGH].astype(BF)
        self.y1o[i + 1, 0] = from_left(val[SUB - 1][:, HIGH], self.strip)
        self.y1e[i + 1, SUB] = from_right(val[0][:, LOW], self.strip)

    def row1(self, i):
        val = self.apply(self.abuf[self.zero + i])
        if i in self.keep:
            val = val * self.keep[i]
        self.z1e[i] = val[..., LOW].astype(BF)
        self.z1o[i, 1:] = val[..., HIGH].astype(BF)
        self.z1o[i, 0] = from_left(val[SUB - 1][:, HIGH], self.strip)

    def row2(self, u):
        val = self.apply(self.abuf[self.zero + u])
        for v, part in enumerate((LOW, HIGH)):
            line = val[..., part]
            self.y2[2 * u + v + 1, 1:SUB + 1] = line.astype(BF)
            self.y2[2 * u + v + 1, 0] = from_left(line[SUB - 1], self.strip)
            self.y2[2 * u + v + 1, SUB + 1] = from_right(line[0], self.strip)

    def row3(self, u):
        val = self.apply(self.abuf[self.zero + u])
        for v, part in enumerate((LOW, HIGH)):
            for q in range(SUB):
                pixel = val[q][:, part]
                if q % 2:
                    self.z2o[2 * u + v + 1, q // 2 + 1] = pixel.astype(BF)
                else:
                    self.z2e[2 * u + v + 1, q // 2] = pixel.astype(BF)
            self.z2o[2 * u + v + 1, 0] = from_left(val[SUB - 1][:, part], self.strip)

    def row4(self, u):
        val = self.apply(self.abuf[self.zero + u])
        for v in range(2):
            line = val[4 * v:4 * v + 4]
            self.y3[2 * u + v + 1, 1:5] = line.astype(BF)
            self.y3[2 * u + v + 1, 0] = side_by_side([from_left(line[3][:, part], self.strip) for part in (LOW, HIGH)])
            self.y3[2 * u + v + 1, 5] = side_by_side([from_right(line[0][:, part], self.strip) for part in (LOW, HIGH)])

    def row5(self, u):
        val = self.apply(self.abuf[self.zero + u])
        for v in range(2):
            for h, part in enumerate((LOW, HIGH)):
                for q in range(4):
                    self.obuf[u, v, h, pl.ds(q, TILE, 4), :] = val[4 * v + q][:, part]
                for w in range(HALVES):
                    self.put(2 * u + w, v, part, self.obuf[u, v, h, 32 * w:32 * w + 32].astype(BF))

    def post(self, layer):
        row, count = ((self.row0, TILE), (self.row1, TILE + 1), (self.row2, SUB), (self.row3, SUB), (self.row4, 4), (self.row5, 4))[layer]
        return [lambda: self.finalize(layer)] + [lambda i=i: row(i) for i in range(count)]


def blend(chunks, rest):
    done = 0
    for n, emit in enumerate(chunks):
        emit()
        goal = len(rest) * (n + 1) // len(chunks)
        for item in rest[done:goal]:
            item()
        done = goal
    for item in rest[done:]:
        item()


def encoder_kernel(image, down1, v1, refine1, v2, down2, v3, refine2, v4, wd3, v5, wr3, v6, out, inbuf, outbuf, in_send, in_recv, out_send, out_recv, taps,
                   vecs, w1, wr1, wd2, wr2, perm, gmat, af, *buffers):
    group = pl.program_id(0)
    me = 2 * lax.axis_index("h") + lax.axis_index("w")

    def peer(k):
        return lax.rem(me + k, PEERS)

    def device(index):
        return {"h": index // 2, "w": lax.rem(index, 2)}

    def images(index, g):
        return pl.ds(index * PAIR * GROUPS + PAIR * g, PAIR)

    def send_in(g, to, sender):
        return pltpu.make_async_remote_copy(image.at[images(to, g)], inbuf.at[g, sender], in_send.at[g, to], in_recv.at[g, sender], device_id=device(to), device_id_type=MESH)

    def keep_in(g):
        return pltpu.make_async_copy(image.at[images(me, g)], inbuf.at[g, me], in_recv.at[g, me])

    def send_out(g, to, sender):
        return pltpu.make_async_remote_copy(outbuf.at[g, to], out.at[images(sender, g)], out_send.at[g, to], out_recv.at[g, sender], device_id=device(to), device_id_type=MESH)

    def keep_out(g):
        return pltpu.make_async_copy(outbuf.at[g, me], out.at[images(me, g)], out_recv.at[g, me])

    def start_out(g):
        for k in range(1, PEERS):
            send_out(g, peer(k), me).start()
        keep_out(g).start()

    @pl.when(group == 0)
    def _():
        barrier = pltpu.get_barrier_semaphore()
        for k in range(1, PEERS):
            pl.semaphore_signal(barrier, inc=1, device_id=device(peer(k)), device_id_type=MESH)
        pl.semaphore_wait(barrier, PEERS - 1)

        def begin(g, _):
            keep_in(g).start()
            for k in range(1, PEERS):
                send_in(g, peer(k), me).start()
            return 0

        lax.fori_loop(0, GROUPS, begin, 0)

        expand_first(down1, taps, w1)
        expand_refine1(refine1, wr1)
        expand_rows(down2, wd2, 2, lambda y, x: 6 * x + y)
        expand_rows(refine2, wr2, 1, lambda y, x: 3 * y + x)
        for i, ref in enumerate((v1, v2, v3, v4, v5, v6)):
            vecs[i] = side_by_side([ref[...]] * (WIDE // ref.shape[1]))
        row, lane = iota((2 * WIDE, LANES), 0), iota((2 * WIDE, LANES), 1)
        for d in range(PHASES):
            perm[:, d * LANES:(d + 1) * LANES] = one_hot(row == 4 * ((lane % TILE) * SUB + lane // TILE) + d - 1)
        row, lane = iota((WIDE, WIDE), 0), iota((WIDE, WIDE), 1)
        for g, rep in enumerate((C1, C2, C3)):
            gmat[g] = one_hot((row % rep) // (rep // SUB) == (lane % rep) // (rep // SUB))
        for e in range(PAIR):
            bs, _, y1e, y1o, _, _, y2, z2e, z2o, y3 = buffers[e:10 * PAIR:PAIR]
            for ref in (y1e, y1o, y2, y3, z2e, z2o, bs):
                ref[0] = jnp.zeros(ref.shape[1:], BF)
            for ref in (y1e, y1o, y2, y3):
                ref[ref.shape[0] - 1] = jnp.zeros(ref.shape[1:], BF)

    @pl.when(group > 0)
    def _():
        start_out(group - 1)

    keep_in(group).wait()
    for k in range(1, PEERS):
        send_in(group, peer(k), peer(k)).wait_recv()

    def put_of(e):
        def put(to, v, part, val):
            outbuf[group, to, e, v, :, part] = val

        return put

    zero = (me + group) // (2 * TILE)
    params = (zero, vecs, gmat, w1, wr1, wd2, wr2, wd3, wr3)
    streams = [Stream(params, buffers[e::PAIR], put_of(e)) for e in range(PAIR)]

    sides = [join([inbuf[group, HALVES * hh + half, e] for e in range(PAIR) for hh in range(4)]) for half in range(HALVES)]
    af[...] = dot(side_by_side(sides), perm[...]).reshape(af.shape)

    def im2col(e, k):
        rows = []
        for c in range(3):
            block = 24 * e + (k // 2) * 6 + c * 2 + k % 2
            rows += [af[block, :, d * LANES:(d + 1) * LANES] for d in range(PHASES)]
        rows.append(jnp.zeros((SUB, LANES), F32))
        streams[e].bs[k + 1] = join(rows).T.astype(BF).reshape(SUB, TILE, LANES)

    gather = [[lambda e=e, k=k: im2col(e, k) for k in range(SUB)] for e in range(PAIR)]
    first, second = streams
    blend([], gather[0])
    blend(first.conv(0), gather[1])
    for layer in range(6):
        blend(second.conv(layer), first.post(layer))
        blend(first.conv(layer + 1) if layer < 5 else [], second.post(layer))

    @pl.when(group == GROUPS - 1)
    def _():
        def sent(g, _):
            for k in range(1, PEERS):
                send_in(g, peer(k), me).wait_send()
            return 0

        lax.fori_loop(0, GROUPS, sent, 0)
        start_out(group)

        def done(g, _):
            for k in range(1, PEERS):
                send_out(g, peer(k), me).wait_send()
                send_out(g, peer(k), peer(k)).wait_recv()
            keep_out(g).wait()
            return 0

        lax.fori_loop(0, GROUPS, done, 0)


def solution(mesh):
    act_spec = P("batch", "h", "w")
    sems = pltpu.SemaphoreType.DMA((GROUPS, PEERS))
    scratch = [
        ((GROUPS, PEERS, PAIR, PIECE_ROWS, PIECE_COLS), BF), ((GROUPS, PEERS, PAIR, 2, 32, WIDE), BF), None, None, None, None, ((32, C1), F32),
        ((6, 3, WIDE), F32), ((WIDE, 512), BF), ((1024, WIDE), BF), ((1152, WIDE), BF), ((1536, WIDE), BF),
        ((512, 640), BF), ((3, WIDE, WIDE), BF), ((48, SUB, 640), F32),
    ]
    for shape, dtype in (
        ((9, SUB, TILE, LANES), BF), ((17, SUB, TILE, WIDE), F32), ((18, 9, TILE, LANES), BF), ((18, 9, TILE, LANES), BF), ((17, 8, TILE, LANES), BF),
        ((17, 9, TILE, LANES), BF), ((18, 10, TILE, LANES), BF), ((17, 4, TILE, LANES), BF), ((17, 5, TILE, LANES), BF), ((10, 6, TILE, WIDE), BF),
        ((4, 2, 2, 64, LANES), F32), ((2, TILE, WIDE), F32), ((2, TILE, WIDE), F32),
    ):
        scratch += [(shape, dtype)] * PAIR

    def local_forward(tile, *params):
        planes = tile.transpose(0, 3, 1, 2).reshape(-1, PIECE_ROWS, PIECE_COLS)
        params = list(params)
        params[8], params[10] = params[8].reshape(-1, WIDE), params[10].reshape(-1, WIDE)
        return pl.pallas_call(
            encoder_kernel,
            grid=(GROUPS,),
            out_shape=jax.ShapeDtypeStruct((128, 2, 32, WIDE), BF),
            in_specs=[pl.BlockSpec(memory_space=pl.ANY)] + [pl.BlockSpec(memory_space=pltpu.VMEM)] * 12,
            out_specs=pl.BlockSpec(memory_space=pl.ANY),
            scratch_shapes=[sems if entry is None else pltpu.VMEM(*entry) for entry in scratch],
            compiler_params=pltpu.CompilerParams(vmem_limit_bytes=60 * 1024 * 1024, collective_id=0, has_side_effects=True),
            name="encoder",
        )(planes, *params)

    return jax.shard_map(local_forward, mesh=mesh, in_specs=(act_spec,) + (P(),) * 12, out_specs=act_spec, check_vma=False)
```

```python
import jax
import jax.numpy as jnp
from jax import lax
from jax.experimental import pallas as pl
from jax.experimental.pallas import tpu as pltpu
from jax.sharding import PartitionSpec as P

NORM_EPS = 1e-5
BF = jnp.bfloat16
F32 = jnp.float32
PAIR, SUB, TILE, LANES, WIDE, UNIT = 2, 8, 16, 128, 256, 128
CHUNK = 2
PEERS, GROUPS, HALVES = 8, 8, 2
C1, C2, C3 = 64, 128, 256
PHASES, PIECE_ROWS, PIECE_COLS = 5, 48, 256
AREAS = (32 * 256, 16 * 128, 8 * 64)
MESH = pl.DeviceIdType.MESH
LOW, HIGH = slice(None, LANES), slice(LANES, None)


def iota(shape, dim):
    return lax.broadcasted_iota(jnp.int32, shape, dim)


def one_hot(mask):
    return jnp.where(mask, 1.0, 0.0).astype(BF)


def join(parts, axis=0):
    return jnp.concatenate(parts, axis=axis)


def side_by_side(parts):
    return jnp.concatenate(parts, axis=1)


def rows_of(ref, index, first, count):
    return ref[index, first:first + count].reshape(count * TILE, ref.shape[-1])


def dot(lhs, rhs):
    return jnp.dot(lhs, rhs, preferred_element_type=F32)


def lane_half(ref, half):
    return ref.at[..., LOW] if half == 0 else ref.at[..., HIGH]


def expand_first(down1, taps, w1):
    taps[...] = jnp.zeros(taps.shape, F32)
    for dy in range(3):
        for dx in range(3):
            taps[pl.ds(9 * dy + 3 * dx, 3), :] = down1[dy, dx].astype(F32)
    source = taps[...].astype(BF)
    row, tap = iota((WIDE, 32), 0), iota((WIDE, 32), 1)
    colour_phase = (row % LANES) // SUB
    colour, phase = colour_phase // PHASES, colour_phase % PHASES
    line = SUB * (row // LANES) + row % SUB
    for o in range(HALVES):
        lanes = []
        for cp in range(HALVES):
            for rp in range(HALVES):
                dy, dx = line - 7 - 4 * o - 2 * rp, phase - 2 * cp
                inside = (dy >= 0) & (dy < 3) & (dx >= 0) & (dx < 3) & (colour < 3)
                lanes.append(dot(one_hot(inside & (tap == 9 * dy + 3 * dx + colour)), source))
        w1[:, o * WIDE:(o + 1) * WIDE] = side_by_side(lanes).astype(BF)


def expand_refine1(refine1, wr1):
    blank = jnp.zeros((C1, C1), BF)
    wr1[...] = jnp.zeros(wr1.shape, BF)
    for dx in range(3):
        for y in range(4):
            pair = side_by_side([refine1[y, dx] if y < 3 else blank, refine1[y - 1, dx] if y else blank])
            for cp in range(HALVES):
                lane_half(wr1, cp)[pl.ds(((y // 2 * 4 + dx + cp) * 2 + y % 2) * C1, C1), :] = pair


def expand_rows(kernel, out, shift, order):
    depth = kernel.shape[2]
    out[...] = jnp.zeros(out.shape, BF)
    for dy in range(3):
        for dx in range(3):
            for r in range(HALVES):
                lane_half(out, r)[pl.ds(order(dy + shift * r, dx) * depth, depth), :] = kernel[dy, dx]


def from_left(tile, strip):
    return jnp.where(strip == 0, 0.0, pltpu.roll(tile, 1, 0)).astype(BF)


def from_right(tile, strip):
    return jnp.where(strip == TILE - 1, 0.0, pltpu.roll(tile, TILE - 1, 0)).astype(BF)


class Stream:
    def __init__(self, params, buffers, put):
        self.put = put
        self.zero, self.vecs, self.gmat, self.w1, self.wr1, self.wd2, self.wr2, self.wd3, self.wr3 = params
        self.bs, self.abuf, self.y1e, self.y1o, self.z1e, self.z1o, self.y2, self.z2e, self.z2o, self.y3, self.obuf, self.sums, self.norm = buffers
        self.strip = iota((TILE, LANES), 0)
        upper = (iota((1, WIDE), 1) % LANES) < C1
        self.keep = {0: jnp.where(upper, 0.0, 1.0), TILE: jnp.where(upper, 1.0, 0.0)}


    def lhs0(self, unit, step):
        return side_by_side([rows_of(self.bs, unit + n, 0, SUB) for n in range(2)])

    def lhs1(self, unit, step):
        return side_by_side([rows_of(ref, unit + step // 2, step % 2, SUB) for ref in (self.y1o, self.y1e)])

    def ninth(self, tile, step):
        return side_by_side([tile(2 * step), tile(2 * step + 1)]) if step < 4 else tile(2 * step)

    def lhs2(self, unit, step):
        taps = ((self.z1o, 0), (self.z1e, 0), (self.z1o, 1))

        def tile(n):
            ref, first = taps[n // 3]
            return rows_of(ref, 2 * unit + n % 3, first, SUB)

        return self.ninth(tile, step)

    def lhs3(self, unit, step):
        return side_by_side([rows_of(self.y2, 2 * unit + n // 3, n % 3, SUB) for n in (2 * step, 2 * step + 1)])

    def lhs4(self, unit, step):
        taps = ((self.z2o, 0), (self.z2e, 0), (self.z2o, 1))

        def tile(n):
            ref, first = taps[n % 3]
            return join([rows_of(ref, 2 * (2 * unit + p) + n // 3, first, 4) for p in range(2)])

        return self.ninth(tile, step)

    def lhs5(self, unit, step):
        return join([rows_of(self.y3, 2 * unit + p + step // 3, step % 3, 4) for p in range(2)])

    def finish(self, layer, unit, val):
        if layer == 1 and unit in self.keep:
            val = val * self.keep[unit]
        tiles = val.reshape(SUB, TILE, WIDE)
        self.abuf[unit] = tiles
        self.total[0] += jnp.sum(tiles, axis=0)
        self.total[1] += jnp.sum(tiles * tiles, axis=0)

    def conv(self, layer):
        lhs = (self.lhs0, self.lhs1, self.lhs2, self.lhs3, self.lhs4, self.lhs5)[layer]
        steps, ref, count = ((1, self.w1, SUB), (4, self.wr1, 15), (5, self.wd2, SUB), (6, self.wr2, SUB), (5, self.wd3, 4), (9, self.wr3, 4))[layer]
        base = 1 if layer == 1 else 0

        waiting = []

        def drain():
            while waiting:
                units, acc = waiting.pop(0)
                for n, unit in enumerate(units):
                    part = acc[n * UNIT:(n + 1) * UNIT]
                    if layer == 0:
                        self.finish(layer, 2 * unit, part[:, :WIDE])
                        self.finish(layer, 2 * unit + 1, part[:, WIDE:])
                    else:
                        self.finish(layer, unit, part)

        def emit(units, first, last):
            rows = side_by_side([join([lhs(unit, step) for unit in units]) for step in range(first, last)])
            acc = dot(rows, ref[first * WIDE:first * WIDE + rows.shape[1], :])
            drain()
            waiting.append((units, acc))

        def chunk(c):
            emit([base + n for n in range(CHUNK * c, min(CHUNK * (c + 1), count))], 0, steps)

        items = [lambda c=c: chunk(c) for c in range(-(-count // CHUNK))]
        if layer == 1:
            items.append(lambda: emit([0], 2, 4))
            items.append(lambda: emit([TILE], 0, 2))

        def start():
            self.total = [jnp.zeros((TILE, WIDE), F32)] * 2

        def store():
            drain()
            for n in range(2):
                self.sums[n] = self.total[n]

        return [start, *items, store]

    def finalize(self, layer):
        rep = (C1, C2, C3)[layer // 2]
        area = AREAS[layer // 2]
        per_strip = area * rep / (WIDE * SUB)
        count = float(area * rep // SUB)
        bias, gain, offset = self.vecs[layer, 0:1, :], self.vecs[layer, 1:2, :], self.vecs[layer, 2:3, :]
        plain, square = [self.sums[n, :SUB] + self.sums[n, SUB:] for n in range(2)]
        rest = join([plain + per_strip * bias, square + 2.0 * bias * plain + per_strip * bias * bias])
        parts = []
        for _ in range(3):
            parts.append(rest.astype(BF))
            rest = rest - parts[-1].astype(F32)
        grouped = dot(join(parts), self.gmat[layer // 2])
        grouped = grouped[:TILE] + grouped[TILE:2 * TILE] + grouped[2 * TILE:]
        mean = jnp.sum(grouped[:SUB], axis=0, keepdims=True) / count
        power = jnp.sum(grouped[SUB:], axis=0, keepdims=True) / count
        scale = lax.rsqrt(jnp.maximum(power - mean * mean, 0.0) + NORM_EPS) * gain
        self.affine = [jnp.broadcast_to(row, (TILE, WIDE)) for row in (scale, offset + (bias - mean) * scale)]

    def apply(self, block):
        return jnp.maximum(block * self.affine[0] + self.affine[1], 0.0)

    def row0(self, i):
        val = self.apply(self.abuf[self.zero + i])
        self.y1e[i + 1, 0:SUB] = val[..., LOW].astype(BF)
        self.y1o[i + 1, 1:] = val[..., HIGH].astype(BF)
        self.y1o[i + 1, 0] = from_left(val[SUB - 1][:, HIGH], self.strip)
        self.y1e[i + 1, SUB] = from_right(val[0][:, LOW], self.strip)

    def row1(self, i):
        val = self.apply(self.abuf[self.zero + i])
        if i in self.keep:
            val = val * self.keep[i]
        self.z1e[i] = val[..., LOW].astype(BF)
        self.z1o[i, 1:] = val[..., HIGH].astype(BF)
        self.z1o[i, 0] = from_left(val[SUB - 1][:, HIGH], self.strip)

    def row2(self, u):
        val = self.apply(self.abuf[self.zero + u])
        for v, part in enumerate((LOW, HIGH)):
            line = val[..., part]
            self.y2[2 * u + v + 1, 1:SUB + 1] = line.astype(BF)
            self.y2[2 * u + v + 1, 0] = from_left(line[SUB - 1], self.strip)
            self.y2[2 * u + v + 1, SUB + 1] = from_right(line[0], self.strip)

    def row3(self, u):
        val = self.apply(self.abuf[self.zero + u])
        for v, part in enumerate((LOW, HIGH)):
            for q in range(SUB):
                pixel = val[q][:, part]
                if q % 2:
                    self.z2o[2 * u + v + 1, q // 2 + 1] = pixel.astype(BF)
                else:
                    self.z2e[2 * u + v + 1, q // 2] = pixel.astype(BF)
            self.z2o[2 * u + v + 1, 0] = from_left(val[SUB - 1][:, part], self.strip)

    def row4(self, u):
        val = self.apply(self.abuf[self.zero + u])
        for v in range(2):
            line = val[4 * v:4 * v + 4]
            self.y3[2 * u + v + 1, 1:5] = line.astype(BF)
            self.y3[2 * u + v + 1, 0] = side_by_side([from_left(line[3][:, part], self.strip) for part in (LOW, HIGH)])
            self.y3[2 * u + v + 1, 5] = side_by_side([from_right(line[0][:, part], self.strip) for part in (LOW, HIGH)])

    def row5(self, u):
        val = self.apply(self.abuf[self.zero + u])
        for v in range(2):
            for h, part in enumerate((LOW, HIGH)):
                for q in range(4):
                    self.obuf[u, v, h, pl.ds(q, TILE, 4), :] = val[4 * v + q][:, part]
                for w in range(HALVES):
                    self.put(2 * u + w, v, part, self.obuf[u, v, h, 32 * w:32 * w + 32].astype(BF))

    def post(self, layer):
        row, count = ((self.row0, TILE), (self.row1, TILE + 1), (self.row2, SUB), (self.row3, SUB), (self.row4, 4), (self.row5, 4))[layer]
        return [lambda: self.finalize(layer)] + [lambda i=i: row(i) for i in range(count)]


def blend(chunks, rest):
    done = 0
    for n, emit in enumerate(chunks):
        emit()
        goal = len(rest) * (n + 1) // len(chunks)
        for item in rest[done:goal]:
            item()
        done = goal
    for item in rest[done:]:
        item()


def encoder_kernel(image, down1, v1, refine1_in, v2, down2_in, v3, refine2_in, v4, wd3_in, v5, wr3_in, v6, out, inbuf, outbuf, in_send, in_recv, out_send, out_recv, taps,
                   refine1, down2, refine2, wd3, wr3, load_sem, vecs, w1, wr1, wd2, wr2, perm, gmat, af, *buffers):
    group = pl.program_id(0)
    me = 2 * lax.axis_index("h") + lax.axis_index("w")

    def peer(k):
        return lax.rem(me + k, PEERS)

    def device(index):
        return {"h": index // 2, "w": lax.rem(index, 2)}

    def images(index, g):
        return pl.ds(index * PAIR * GROUPS + PAIR * g, PAIR)

    def send_in(g, to, sender):
        return pltpu.make_async_remote_copy(image.at[images(to, g)], inbuf.at[g, sender], in_send.at[g, to], in_recv.at[g, sender], device_id=device(to), device_id_type=MESH)

    def keep_in(g):
        return pltpu.make_async_copy(image.at[images(me, g)], inbuf.at[g, me], in_recv.at[g, me])

    def send_out(g, to, sender):
        return pltpu.make_async_remote_copy(outbuf.at[g, to], out.at[images(sender, g)], out_send.at[g, to], out_recv.at[g, sender], device_id=device(to), device_id_type=MESH)

    def keep_out(g):
        return pltpu.make_async_copy(outbuf.at[g, me], out.at[images(me, g)], out_recv.at[g, me])

    def start_out(g):
        for k in range(1, PEERS):
            send_out(g, peer(k), me).start()
        keep_out(g).start()

    def wait_in(g):
        keep_in(g).wait()
        for k in range(1, PEERS):
            send_in(g, peer(k), peer(k)).wait_recv()

    def put_of(e):
        def put(to, v, part, val):
            outbuf[group, to, e, v, :, part] = val

        return put

    zero = (me + group) // (2 * TILE)
    params = (zero, vecs, gmat, w1, wr1, wd2, wr2, wd3, wr3)
    streams = [Stream(params, buffers[e::PAIR], put_of(e)) for e in range(PAIR)]

    def permute(g):
        sides = [join([inbuf[g, HALVES * hh + half, e] for e in range(PAIR) for hh in range(4)]) for half in range(HALVES)]
        af[...] = dot(side_by_side(sides), perm[...]).reshape(af.shape)

    def im2col(e, k):
        rows = []
        for c in range(3):
            block = 24 * e + (k // 2) * 6 + c * 2 + k % 2
            rows += [af[block, :, d * LANES:(d + 1) * LANES] for d in range(PHASES)]
        rows.append(jnp.zeros((SUB, LANES), F32))
        streams[e].bs[k + 1] = join(rows).T.astype(BF).reshape(SUB, TILE, LANES)

    gather = [[lambda e=e, k=k: im2col(e, k) for k in range(SUB)] for e in range(PAIR)]

    @pl.when(group == 0)
    def _():
        pairs = ((refine1_in, refine1), (down2_in, down2), (refine2_in, refine2), (wd3_in, wd3), (wr3_in, wr3))
        loads = [pltpu.make_async_copy(*pair, load_sem.at[n]) for n, pair in enumerate(pairs)]
        for load in loads:
            load.start()
        barrier = pltpu.get_barrier_semaphore()
        for k in range(1, PEERS):
            pl.semaphore_signal(barrier, inc=1, device_id=device(peer(k)), device_id_type=MESH)
        pl.semaphore_wait(barrier, PEERS - 1)

        def begin(g, _):
            keep_in(g).start()
            for k in range(1, PEERS):
                send_in(g, peer(k), me).start()
            return 0

        lax.fori_loop(0, GROUPS, begin, 0)

        expand_first(down1, taps, w1)
        for load in loads:
            load.wait()
        expand_refine1(refine1, wr1)
        expand_rows(down2, wd2, 2, lambda y, x: 6 * x + y)
        expand_rows(refine2, wr2, 1, lambda y, x: 3 * y + x)
        for i, ref in enumerate((v1, v2, v3, v4, v5, v6)):
            vecs[i, 0:3] = side_by_side([ref[...]] * (WIDE // ref.shape[1]))
        row, lane = iota((2 * WIDE, LANES), 0), iota((2 * WIDE, LANES), 1)
        for d in range(PHASES):
            perm[:, d * LANES:(d + 1) * LANES] = one_hot(row == 4 * ((lane % TILE) * SUB + lane // TILE) + d - 1)
        row, lane = iota((WIDE, WIDE), 0), iota((WIDE, WIDE), 1)
        for g, rep in enumerate((C1, C2, C3)):
            gmat[g] = one_hot((row % rep) // (rep // SUB) == (lane % rep) // (rep // SUB))
        for e in range(PAIR):
            bs, _, y1e, y1o, _, _, y2, z2e, z2o, y3 = buffers[e:10 * PAIR:PAIR]
            for ref in (y1e, y1o, y2, y3, z2e, z2o, bs):
                ref[0] = jnp.zeros(ref.shape[1:], BF)
            for ref, last in ((y1e, 17), (y1o, 17), (y2, 17), (y3, 9)):
                ref[last] = jnp.zeros(ref.shape[1:], BF)

        wait_in(0)
        permute(0)
        for item in (*gather[0], *gather[1], *streams[0].conv(0)):
            item()

    @pl.when(group > 0)
    def _():
        start_out(group - 1)

    first, second = streams
    following = lax.rem(group + 1, GROUPS)
    for layer in range(6):
        extra = gather[0] + gather[1] if layer == 5 else []
        blend(second.conv(layer), first.post(layer) + extra)
        if layer == 4:
            pl.when(group < GROUPS - 1)(lambda: wait_in(following))
        extra = [lambda: permute(following)] if layer == 4 else []
        blend(extra + first.conv(layer + 1 if layer < 5 else 0), second.post(layer))

    @pl.when(group == GROUPS - 1)
    def _():
        def sent(g, _):
            for k in range(1, PEERS):
                send_in(g, peer(k), me).wait_send()
            return 0

        lax.fori_loop(0, GROUPS, sent, 0)
        start_out(group)

        def done(g, _):
            for k in range(1, PEERS):
                send_out(g, peer(k), me).wait_send()
                send_out(g, peer(k), peer(k)).wait_recv()
            keep_out(g).wait()
            return 0

        lax.fori_loop(0, GROUPS, done, 0)


def solution(mesh):
    act_spec = P("batch", "h", "w")
    sems = pltpu.SemaphoreType.DMA((GROUPS, PEERS))
    scratch = [
        ((GROUPS, PEERS, PAIR, PIECE_ROWS, PIECE_COLS), BF), ((GROUPS, PEERS, PAIR, 2, 32, WIDE), BF), sems, sems, sems, sems, ((32, C1), F32),
        ((3, 3, C1, C1), BF), ((3, 3, C1, C2), BF), ((3, 3, C2, C2), BF), ((1152, WIDE), BF), ((2304, WIDE), BF), pltpu.SemaphoreType.DMA((5,)),
        ((8, 8, WIDE), F32), ((WIDE, 512), BF), ((1024, WIDE), BF), ((1152, WIDE), BF), ((1536, WIDE), BF),
        ((512, 640), BF), ((3, WIDE, WIDE), BF), ((48, SUB, 640), F32),
    ]
    for shape, dtype in (
        ((9, SUB, TILE, LANES), BF), ((17, SUB, TILE, WIDE), F32), ((20, 9, TILE, LANES), BF), ((20, 9, TILE, LANES), BF), ((17, 8, TILE, LANES), BF),
        ((20, 9, TILE, LANES), BF), ((18, 10, TILE, LANES), BF), ((17, 4, TILE, LANES), BF), ((20, 5, TILE, LANES), BF), ((10, 6, TILE, WIDE), BF),
        ((4, 2, 2, 64, LANES), F32), ((2, TILE, WIDE), F32), ((2, TILE, WIDE), F32),
    ):
        scratch += [(shape, dtype)] * PAIR

    def local_forward(tile, *params):
        planes = tile.transpose(0, 3, 1, 2).reshape(-1, PIECE_ROWS, PIECE_COLS)
        params = list(params)
        params[8], params[10] = params[8].reshape(-1, WIDE), params[10].reshape(-1, WIDE)
        result = pl.pallas_call(
            encoder_kernel,
            grid=(GROUPS,),
            out_shape=jax.ShapeDtypeStruct((128, 2, 32, WIDE), BF),
            in_specs=[pl.BlockSpec(memory_space=pltpu.HBM if n in (0, 3, 5, 7, 9, 11) else pltpu.VMEM) for n in range(13)],
            out_specs=pl.BlockSpec(memory_space=pl.ANY),
            scratch_shapes=[pltpu.VMEM(*entry) if isinstance(entry, tuple) else entry for entry in scratch],
            compiler_params=pltpu.CompilerParams(vmem_limit_bytes=60 * 1024 * 1024, collective_id=0, has_side_effects=True),
            name="encoder",
        )(planes, *params)
        return jnp.maximum(result, 0)

    return jax.shard_map(local_forward, mesh=mesh, in_specs=(act_spec,) + (P(),) * 12, out_specs=act_spec, check_vma=False)
```

```python
import jax
import jax.numpy as jnp
from jax import lax
from jax.experimental import pallas as pl
from jax.experimental.pallas import tpu as pltpu
from jax.sharding import PartitionSpec as P

NORM_EPS = 1e-5
BF = jnp.bfloat16
F32 = jnp.float32
PAIR, SUB, TILE, LANES, WIDE, UNIT = 2, 8, 16, 128, 256, 128
CHUNK = 2
PEERS, GROUPS, HALVES = 8, 8, 2
C1, C2, C3 = 64, 128, 256
PHASES, PIECE_ROWS, PIECE_COLS = 5, 48, 256
AREAS = (32 * 256, 16 * 128, 8 * 64)
MESH = pl.DeviceIdType.MESH
LOW, HIGH = slice(None, LANES), slice(LANES, None)


def iota(shape, dim):
    return lax.broadcasted_iota(jnp.int32, shape, dim)


def one_hot(mask):
    return jnp.where(mask, 1.0, 0.0).astype(BF)


def join(parts, axis=0):
    return jnp.concatenate(parts, axis=axis)


def side_by_side(parts):
    return jnp.concatenate(parts, axis=1)


def rows_of(ref, index, first, count):
    return ref[index, first:first + count].reshape(count * TILE, ref.shape[-1])


def dot(lhs, rhs):
    return jnp.dot(lhs, rhs, preferred_element_type=F32)


def lane_half(ref, half):
    return ref.at[..., LOW] if half == 0 else ref.at[..., HIGH]


def expand_first(down1, taps, w1):
    taps[...] = jnp.zeros(taps.shape, F32)
    for dy in range(3):
        for dx in range(3):
            taps[pl.ds(9 * dy + 3 * dx, 3), :] = down1[dy, dx].astype(F32)
    source = taps[...].astype(BF)
    row, tap = iota((WIDE, 32), 0), iota((WIDE, 32), 1)
    colour_phase = (row % LANES) // SUB
    colour, phase = colour_phase // PHASES, colour_phase % PHASES
    line = SUB * (row // LANES) + row % SUB
    for o in range(HALVES):
        lanes = []
        for cp in range(HALVES):
            for rp in range(HALVES):
                dy, dx = line - 7 - 4 * o - 2 * rp, phase - 2 * cp
                inside = (dy >= 0) & (dy < 3) & (dx >= 0) & (dx < 3) & (colour < 3)
                lanes.append(dot(one_hot(inside & (tap == 9 * dy + 3 * dx + colour)), source))
        w1[:, o * WIDE:(o + 1) * WIDE] = side_by_side(lanes).astype(BF)


def expand_refine1(refine1, wr1):
    blank = jnp.zeros((C1, C1), BF)
    wr1[...] = jnp.zeros(wr1.shape, BF)
    for dx in range(3):
        for y in range(4):
            pair = side_by_side([refine1[y, dx] if y < 3 else blank, refine1[y - 1, dx] if y else blank])
            for cp in range(HALVES):
                lane_half(wr1, cp)[pl.ds(((y // 2 * 4 + dx + cp) * 2 + y % 2) * C1, C1), :] = pair


def expand_rows(kernel, out, shift, order):
    depth = kernel.shape[2]
    out[...] = jnp.zeros(out.shape, BF)
    for dy in range(3):
        for dx in range(3):
            for r in range(HALVES):
                lane_half(out, r)[pl.ds(order(dy + shift * r, dx) * depth, depth), :] = kernel[dy, dx]


def from_left(tile, strip):
    return jnp.where(strip == 0, 0.0, pltpu.roll(tile, 1, 0)).astype(BF)


def from_right(tile, strip):
    return jnp.where(strip == TILE - 1, 0.0, pltpu.roll(tile, TILE - 1, 0)).astype(BF)


class Stream:
    def __init__(self, params, buffers, put):
        self.put = put
        self.zero, self.vecs, self.gmat, self.w1, self.wr1, self.wd2, self.wr2, self.wd3, self.wr3 = params
        self.bs, self.abuf, self.y1e, self.y1o, self.z1e, self.z1o, self.y2, self.z2e, self.z2o, self.y3, self.obuf, self.sums, self.z1m = buffers
        self.strip = iota((TILE, LANES), 0)
        self.lane = iota((TILE, LANES), 1)
        upper = (iota((1, WIDE), 1) % LANES) < C1
        self.keep = {0: jnp.where(upper, 0.0, 1.0), TILE: jnp.where(upper, 1.0, 0.0)}


    def lhs0(self, unit, step):
        return side_by_side([rows_of(self.bs, unit + n, 0, SUB) for n in range(2)])

    def lhs1(self, unit, step):
        return side_by_side([rows_of(ref, unit + step // 2, step % 2, SUB) for ref in (self.y1o, self.y1e)])

    def ninth(self, tile, step):
        return side_by_side([tile(2 * step), tile(2 * step + 1)]) if step < 4 else tile(2 * step)

    def lhs2(self, unit, step):
        if step < 3:
            ref, first = ((self.z1o, 0), (self.z1e, 0), (self.z1o, 1))[step]
            return side_by_side([rows_of(ref, 2 * unit + n, first, SUB) for n in range(2)])
        return side_by_side([rows_of(self.z1m, unit, 0, SUB), rows_of(self.z1o, 2 * unit + 2, 1, SUB)])

    def lhs3(self, unit, step):
        return side_by_side([rows_of(self.y2, 2 * unit + n // 3, n % 3, SUB) for n in (2 * step, 2 * step + 1)])

    def lhs4(self, unit, step):
        taps = ((self.z2o, 0), (self.z2e, 0), (self.z2o, 1))

        def tile(n):
            ref, first = taps[n % 3]
            return join([rows_of(ref, 2 * (2 * unit + p) + n // 3, first, 4) for p in range(2)])

        return self.ninth(tile, step)

    def lhs5(self, unit, step):
        return join([rows_of(self.y3, 2 * unit + p + step // 3, step % 3, 4) for p in range(2)])

    def finish(self, layer, unit, val):
        if layer == 1 and unit in self.keep:
            val = val * self.keep[unit]
        tiles = val.reshape(SUB, TILE, WIDE)
        self.abuf[unit] = tiles
        self.total[0] += jnp.sum(tiles, axis=0)
        self.total[1] += jnp.sum(tiles * tiles, axis=0)

    def conv(self, layer):
        lhs = (self.lhs0, self.lhs1, self.lhs2, self.lhs3, self.lhs4, self.lhs5)[layer]
        steps, ref, count = ((1, self.w1, SUB), (4, self.wr1, 15), (4, self.wd2, SUB), (6, self.wr2, SUB), (5, self.wd3, 4), (9, self.wr3, 4))[layer]
        base = 1 if layer == 1 else 0

        waiting = []

        def drain():
            while waiting:
                units, acc = waiting.pop(0)
                for n, unit in enumerate(units):
                    part = acc[n * UNIT:(n + 1) * UNIT]
                    if layer == 0:
                        self.finish(layer, 2 * unit, part[:, :WIDE])
                        self.finish(layer, 2 * unit + 1, part[:, WIDE:])
                    else:
                        self.finish(layer, unit, part)

        def emit(units, first, last):
            rows = side_by_side([join([lhs(unit, step) for unit in units]) for step in range(first, last)])
            acc = dot(rows, ref[first * WIDE:first * WIDE + rows.shape[1], :])
            drain()
            waiting.append((units, acc))

        def chunk(c):
            emit([base + n for n in range(CHUNK * c, min(CHUNK * (c + 1), count))], 0, steps)

        items = [lambda c=c: chunk(c) for c in range(-(-count // CHUNK))]
        if layer == 1:
            items.append(lambda: emit([0], 2, 4))
            items.append(lambda: emit([TILE], 0, 2))

        def start():
            self.total = [jnp.zeros((TILE, WIDE), F32)] * 2

        def store():
            drain()
            for n in range(2):
                self.sums[n] = self.total[n]

        return [start, *items, store]

    def finalize(self, layer):
        rep = (C1, C2, C3)[layer // 2]
        area = AREAS[layer // 2]
        per_strip = area * rep / (WIDE * SUB)
        count = float(area * rep // SUB)
        bias, gain, offset = self.vecs[layer, 0:1, :], self.vecs[layer, 1:2, :], self.vecs[layer, 2:3, :]
        plain, square = [self.sums[n, :SUB] + self.sums[n, SUB:] for n in range(2)]
        rest = join([plain + per_strip * bias, square + 2.0 * bias * plain + per_strip * bias * bias])
        parts = []
        for _ in range(3):
            parts.append(rest.astype(BF))
            rest = rest - parts[-1].astype(F32)
        grouped = dot(join(parts), self.gmat[layer // 2])
        grouped = grouped[:TILE] + grouped[TILE:2 * TILE] + grouped[2 * TILE:]
        mean = jnp.sum(grouped[:SUB], axis=0, keepdims=True) / count
        power = jnp.sum(grouped[SUB:], axis=0, keepdims=True) / count
        scale = lax.rsqrt(jnp.maximum(power - mean * mean, 0.0) + NORM_EPS) * gain
        self.affine = [jnp.broadcast_to(row, (TILE, WIDE)) for row in (scale, offset + (bias - mean) * scale)]

    def apply(self, block):
        return jnp.maximum(block * self.affine[0] + self.affine[1], 0.0)

    def row0(self, i):
        val = self.apply(self.abuf[self.zero + i])
        self.y1e[i + 1, 0:SUB] = val[..., LOW].astype(BF)
        self.y1o[i + 1, 1:] = val[..., HIGH].astype(BF)
        self.y1o[i + 1, 0] = from_left(val[SUB - 1][:, HIGH], self.strip)
        self.y1e[i + 1, SUB] = from_right(val[0][:, LOW], self.strip)

    def row1(self, i):
        val = self.apply(self.abuf[self.zero + i])
        if i in self.keep:
            val = val * self.keep[i]
        self.z1e[i] = val[..., LOW].astype(BF)
        self.z1o[i, 1:] = val[..., HIGH].astype(BF)
        edge = from_left(val[SUB - 1][:, HIGH], self.strip)
        self.z1o[i, 0] = edge
        if i and i % 2 == 0:
            for q in range(SUB):
                left = val[q - 1][:, HIGH] if q else edge.astype(F32)
                shifted = pltpu.roll(val[q][:, LOW], C1, 1)
                self.z1m[i // 2 - 1, q] = jnp.where(self.lane < C1, left, shifted).astype(BF)

    def row2(self, u):
        val = self.apply(self.abuf[self.zero + u])
        for v, part in enumerate((LOW, HIGH)):
            line = val[..., part]
            self.y2[2 * u + v + 1, 1:SUB + 1] = line.astype(BF)
            self.y2[2 * u + v + 1, 0] = from_left(line[SUB - 1], self.strip)
            self.y2[2 * u + v + 1, SUB + 1] = from_right(line[0], self.strip)

    def row3(self, u):
        val = self.apply(self.abuf[self.zero + u])
        for v, part in enumerate((LOW, HIGH)):
            for q in range(SUB):
                pixel = val[q][:, part]
                if q % 2:
                    self.z2o[2 * u + v + 1, q // 2 + 1] = pixel.astype(BF)
                else:
                    self.z2e[2 * u + v + 1, q // 2] = pixel.astype(BF)
            self.z2o[2 * u + v + 1, 0] = from_left(val[SUB - 1][:, part], self.strip)

    def row4(self, u):
        val = self.apply(self.abuf[self.zero + u])
        for v in range(2):
            line = val[4 * v:4 * v + 4]
            self.y3[2 * u + v + 1, 1:5] = line.astype(BF)
            self.y3[2 * u + v + 1, 0] = side_by_side([from_left(line[3][:, part], self.strip) for part in (LOW, HIGH)])
            self.y3[2 * u + v + 1, 5] = side_by_side([from_right(line[0][:, part], self.strip) for part in (LOW, HIGH)])

    def row5(self, u):
        val = self.apply(self.abuf[self.zero + u])
        for v in range(2):
            for h, part in enumerate((LOW, HIGH)):
                for q in range(4):
                    self.obuf[u, v, h, pl.ds(q, TILE, 4), :] = val[4 * v + q][:, part]
                for w in range(HALVES):
                    self.put(2 * u + w, v, part, self.obuf[u, v, h, 32 * w:32 * w + 32].astype(BF))

    def post(self, layer):
        row, count = ((self.row0, TILE), (self.row1, TILE + 1), (self.row2, SUB), (self.row3, SUB), (self.row4, 4), (self.row5, 4))[layer]
        return [lambda: self.finalize(layer)] + [lambda i=i: row(i) for i in range(count)]


def blend(chunks, rest):
    done = 0
    for n, emit in enumerate(chunks):
        emit()
        goal = len(rest) * (n + 1) // len(chunks)
        for item in rest[done:goal]:
            item()
        done = goal
    for item in rest[done:]:
        item()


def encoder_kernel(image, down1, v1, refine1_in, v2, down2_in, v3, refine2_in, v4, wd3_in, v5, wr3_in, v6, out, inbuf, outbuf, in_send, in_recv, out_send, out_recv, taps,
                   refine1, down2, refine2, wd3, wr3, load_sem, vecs, w1, wr1, wd2, wr2, perm, gmat, af, *buffers):
    group = pl.program_id(0)
    me = 2 * lax.axis_index("h") + lax.axis_index("w")

    def peer(k):
        return lax.rem(me + k, PEERS)

    def device(index):
        return {"h": index // 2, "w": lax.rem(index, 2)}

    def images(index, g):
        return pl.ds(index * PAIR * GROUPS + PAIR * g, PAIR)

    def send_in(g, to, sender):
        return pltpu.make_async_remote_copy(image.at[images(to, g)], inbuf.at[g, sender], in_send.at[g, to], in_recv.at[g, sender], device_id=device(to), device_id_type=MESH)

    def keep_in(g):
        return pltpu.make_async_copy(image.at[images(me, g)], inbuf.at[g, me], in_recv.at[g, me])

    def send_out(g, to, sender):
        return pltpu.make_async_remote_copy(outbuf.at[g, to], out.at[images(sender, g)], out_send.at[g, to], out_recv.at[g, sender], device_id=device(to), device_id_type=MESH)

    def keep_out(g):
        return pltpu.make_async_copy(outbuf.at[g, me], out.at[images(me, g)], out_recv.at[g, me])

    def start_out(g):
        for k in range(1, PEERS):
            send_out(g, peer(k), me).start()
        keep_out(g).start()

    def wait_in(g):
        keep_in(g).wait()
        for k in range(1, PEERS):
            send_in(g, peer(k), peer(k)).wait_recv()

    def put_of(e):
        def put(to, v, part, val):
            outbuf[group, to, e, v, :, part] = val

        return put

    zero = (me + group) // (2 * TILE)
    params = (zero, vecs, gmat, w1, wr1, wd2, wr2, wd3, wr3)
    streams = [Stream(params, buffers[e::PAIR], put_of(e)) for e in range(PAIR)]

    def permute(g):
        sides = [join([inbuf[g, HALVES * hh + half, e] for e in range(PAIR) for hh in range(4)]) for half in range(HALVES)]
        af[...] = dot(side_by_side(sides), perm[...]).reshape(af.shape)

    def im2col(e, k):
        rows = []
        for c in range(3):
            block = 24 * e + (k // 2) * 6 + c * 2 + k % 2
            rows += [af[block, :, d * LANES:(d + 1) * LANES] for d in range(PHASES)]
        rows.append(jnp.zeros((SUB, LANES), F32))
        streams[e].bs[k + 1] = join(rows).T.astype(BF).reshape(SUB, TILE, LANES)

    gather = [[lambda e=e, k=k: im2col(e, k) for k in range(SUB)] for e in range(PAIR)]

    @pl.when(group == 0)
    def _():
        pairs = ((refine1_in, refine1), (down2_in, down2), (refine2_in, refine2), (wd3_in, wd3), (wr3_in, wr3))
        loads = [pltpu.make_async_copy(*pair, load_sem.at[n]) for n, pair in enumerate(pairs)]
        for load in loads:
            load.start()
        barrier = pltpu.get_barrier_semaphore()
        for k in range(1, PEERS):
            pl.semaphore_signal(barrier, inc=1, device_id=device(peer(k)), device_id_type=MESH)
        pl.semaphore_wait(barrier, PEERS - 1)

        def begin(g, _):
            keep_in(g).start()
            for k in range(1, PEERS):
                send_in(g, peer(k), me).start()
            return 0

        lax.fori_loop(0, GROUPS, begin, 0)

        expand_first(down1, taps, w1)
        for load in loads:
            load.wait()
        expand_refine1(refine1, wr1)
        expand_rows(down2, wd2, 2, lambda y, x: 4 * x + y if y < 4 else 12 + x)
        expand_rows(refine2, wr2, 1, lambda y, x: 3 * y + x)
        for i, ref in enumerate((v1, v2, v3, v4, v5, v6)):
            vecs[i, 0:3] = side_by_side([ref[...]] * (WIDE // ref.shape[1]))
        row, lane = iota((2 * WIDE, LANES), 0), iota((2 * WIDE, LANES), 1)
        for d in range(PHASES):
            perm[:, d * LANES:(d + 1) * LANES] = one_hot(row == 4 * ((lane % TILE) * SUB + lane // TILE) + d - 1)
        row, lane = iota((WIDE, WIDE), 0), iota((WIDE, WIDE), 1)
        for g, rep in enumerate((C1, C2, C3)):
            gmat[g] = one_hot((row % rep) // (rep // SUB) == (lane % rep) // (rep // SUB))
        for e in range(PAIR):
            bs, _, y1e, y1o, _, _, y2, z2e, z2o, y3 = buffers[e:10 * PAIR:PAIR]
            for ref in (y1e, y1o, y2, y3, z2e, z2o, bs):
                ref[0] = jnp.zeros(ref.shape[1:], BF)
            for ref, last in ((y1e, 17), (y1o, 17), (y2, 17), (y3, 9)):
                ref[last] = jnp.zeros(ref.shape[1:], BF)

        wait_in(0)
        permute(0)
        for item in (*gather[0], *gather[1], *streams[0].conv(0)):
            item()

    @pl.when(group > 0)
    def _():
        start_out(group - 1)

    first, second = streams
    following = lax.rem(group + 1, GROUPS)
    for layer in range(6):
        extra = gather[0] + gather[1] if layer == 5 else []
        blend(second.conv(layer), first.post(layer) + extra)
        if layer == 4:
            pl.when(group < GROUPS - 1)(lambda: wait_in(following))
        extra = [lambda: permute(following)] if layer == 4 else []
        blend(extra + first.conv(layer + 1 if layer < 5 else 0), second.post(layer))

    @pl.when(group == GROUPS - 1)
    def _():
        def sent(g, _):
            for k in range(1, PEERS):
                send_in(g, peer(k), me).wait_send()
            return 0

        lax.fori_loop(0, GROUPS, sent, 0)
        start_out(group)

        def done(g, _):
            for k in range(1, PEERS):
                send_out(g, peer(k), me).wait_send()
                send_out(g, peer(k), peer(k)).wait_recv()
            keep_out(g).wait()
            return 0

        lax.fori_loop(0, GROUPS, done, 0)


def solution(mesh):
    act_spec = P("batch", "h", "w")
    sems = pltpu.SemaphoreType.DMA((GROUPS, PEERS))
    scratch = [
        ((GROUPS, PEERS, PAIR, PIECE_ROWS, PIECE_COLS), BF), ((GROUPS, PEERS, PAIR, 2, 32, WIDE), BF), sems, sems, sems, sems, ((32, C1), F32),
        ((3, 3, C1, C1), BF), ((3, 3, C1, C2), BF), ((3, 3, C2, C2), BF), ((1152, WIDE), BF), ((2304, WIDE), BF), pltpu.SemaphoreType.DMA((5,)),
        ((8, 8, WIDE), F32), ((WIDE, 512), BF), ((1024, WIDE), BF), ((1024, WIDE), BF), ((1536, WIDE), BF),
        ((512, 640), BF), ((3, WIDE, WIDE), BF), ((48, SUB, 640), F32),
    ]
    for shape, dtype in (
        ((9, SUB, TILE, LANES), BF), ((17, SUB, TILE, WIDE), F32), ((20, 9, TILE, LANES), BF), ((20, 9, TILE, LANES), BF), ((17, 8, TILE, LANES), BF),
        ((20, 9, TILE, LANES), BF), ((18, 10, TILE, LANES), BF), ((17, 4, TILE, LANES), BF), ((20, 5, TILE, LANES), BF), ((10, 6, TILE, WIDE), BF),
        ((4, 2, 2, 64, LANES), F32), ((2, TILE, WIDE), F32), ((8, SUB, TILE, LANES), BF),
    ):
        scratch += [(shape, dtype)] * PAIR

    def local_forward(tile, *params):
        planes = tile.transpose(0, 3, 1, 2).reshape(-1, PIECE_ROWS, PIECE_COLS)
        params = list(params)
        params[8], params[10] = params[8].reshape(-1, WIDE), params[10].reshape(-1, WIDE)
        result = pl.pallas_call(
            encoder_kernel,
            grid=(GROUPS,),
            out_shape=jax.ShapeDtypeStruct((128, 2, 32, WIDE), BF),
            in_specs=[pl.BlockSpec(memory_space=pltpu.HBM if n in (0, 3, 5, 7, 9, 11) else pltpu.VMEM) for n in range(13)],
            out_specs=pl.BlockSpec(memory_space=pl.ANY),
            scratch_shapes=[pltpu.VMEM(*entry) if isinstance(entry, tuple) else entry for entry in scratch],
            compiler_params=pltpu.CompilerParams(vmem_limit_bytes=60 * 1024 * 1024, collective_id=0, has_side_effects=True),
            name="encoder",
        )(planes, *params)
        return jnp.maximum(result, 0)

    return jax.shard_map(local_forward, mesh=mesh, in_specs=(act_spec,) + (P(),) * 12, out_specs=act_spec, check_vma=False)
```

```python
import jax
import jax.numpy as jnp
from jax import lax
from jax.experimental import pallas as pl
from jax.experimental.pallas import tpu as pltpu
from jax.sharding import PartitionSpec as P

NORM_EPS = 1e-5
BF = jnp.bfloat16
F32 = jnp.float32
PAIR, SUB, TILE, LANES, WIDE, UNIT = 2, 8, 16, 128, 256, 128
CHUNK = 2
PEERS, GROUPS, HALVES = 8, 8, 2
C1, C2, C3 = 64, 128, 256
PHASES, PIECE_ROWS, PIECE_COLS = 5, 48, 256
AREAS = (32 * 256, 16 * 128, 8 * 64)
MESH = pl.DeviceIdType.MESH
LOW, HIGH = slice(None, LANES), slice(LANES, None)


def iota(shape, dim):
    return lax.broadcasted_iota(jnp.int32, shape, dim)


def one_hot(mask):
    return jnp.where(mask, 1.0, 0.0).astype(BF)


def join(parts, axis=0):
    return jnp.concatenate(parts, axis=axis)


def side_by_side(parts):
    return jnp.concatenate(parts, axis=1)


def rows_of(ref, index, first, count):
    return ref[index, first:first + count].reshape(count * TILE, ref.shape[-1])


def dot(lhs, rhs):
    return jnp.dot(lhs, rhs, preferred_element_type=F32)


def lane_half(ref, half):
    return ref.at[..., LOW] if half == 0 else ref.at[..., HIGH]


def expand_first(down1, taps, w1):
    taps[...] = jnp.zeros(taps.shape, F32)
    for dy in range(3):
        for dx in range(3):
            taps[pl.ds(9 * dy + 3 * dx, 3), :] = down1[dy, dx].astype(F32)
    source = taps[...].astype(BF)
    row, tap = iota((WIDE, 32), 0), iota((WIDE, 32), 1)
    colour_phase = (row % LANES) // SUB
    colour, phase = colour_phase // PHASES, colour_phase % PHASES
    line = SUB * (row // LANES) + row % SUB
    for o in range(HALVES):
        lanes = []
        for cp in range(HALVES):
            for rp in range(HALVES):
                dy, dx = line - 7 - 4 * o - 2 * rp, phase - 2 * cp
                inside = (dy >= 0) & (dy < 3) & (dx >= 0) & (dx < 3) & (colour < 3)
                lanes.append(dot(one_hot(inside & (tap == 9 * dy + 3 * dx + colour)), source))
        w1[:, o * WIDE:(o + 1) * WIDE] = side_by_side(lanes).astype(BF)


def expand_refine1(refine1, wr1):
    blank = jnp.zeros((C1, C1), BF)
    wr1[...] = jnp.zeros(wr1.shape, BF)
    for dx in range(3):
        for y in range(4):
            pair = side_by_side([refine1[y, dx] if y < 3 else blank, refine1[y - 1, dx] if y else blank])
            for cp in range(HALVES):
                lane_half(wr1, cp)[pl.ds(((y // 2 * 4 + dx + cp) * 2 + y % 2) * C1, C1), :] = pair


def expand_rows(kernel, out, shift, order):
    depth = kernel.shape[2]
    out[...] = jnp.zeros(out.shape, BF)
    for dy in range(3):
        for dx in range(3):
            for r in range(HALVES):
                lane_half(out, r)[pl.ds(order(dy + shift * r, dx) * depth, depth), :] = kernel[dy, dx]


def from_left(tile, strip):
    return jnp.where(strip == 0, 0.0, pltpu.roll(tile, 1, 0)).astype(BF)


def from_right(tile, strip):
    return jnp.where(strip == TILE - 1, 0.0, pltpu.roll(tile, TILE - 1, 0)).astype(BF)


class Stream:
    def __init__(self, params, buffers, put):
        self.put = put
        self.zero, self.vecs, self.gmat, self.w1, self.wr1, self.wd2, self.wr2, self.wd3, self.wr3 = params
        self.bs, self.abuf, self.y1e, self.y1o, self.z1e, self.z1o, self.y2, self.z2e, self.z2o, self.y3, self.obuf, self.sums, self.z1m = buffers
        self.strip = iota((TILE, LANES), 0)
        self.lane = iota((TILE, LANES), 1)
        upper = (iota((1, WIDE), 1) % LANES) < C1
        self.keep = {0: jnp.where(upper, 0.0, 1.0), TILE: jnp.where(upper, 1.0, 0.0)}


    def lhs0(self, unit, step):
        return side_by_side([rows_of(self.bs, unit + n, 0, SUB) for n in range(2)])

    def lhs1(self, unit, step):
        return side_by_side([rows_of(ref, unit + step // 2, step % 2, SUB) for ref in (self.y1o, self.y1e)])

    def ninth(self, tile, step):
        return side_by_side([tile(2 * step), tile(2 * step + 1)]) if step < 4 else tile(2 * step)

    def lhs2(self, unit, step):
        if step < 3:
            ref, first = ((self.z1o, 0), (self.z1e, 0), (self.z1o, 1))[step]
            return side_by_side([rows_of(ref, 2 * unit + n, first, SUB) for n in range(2)])
        return side_by_side([rows_of(self.z1m, unit, 0, SUB), rows_of(self.z1o, 2 * unit + 2, 1, SUB)])

    def lhs3(self, unit, step):
        return side_by_side([rows_of(self.y2, 2 * unit + n // 3, n % 3, SUB) for n in (2 * step, 2 * step + 1)])

    def lhs4(self, unit, step):
        taps = ((self.z2o, 0), (self.z2e, 0), (self.z2o, 1))

        def tile(n):
            ref, first = taps[n % 3]
            return join([rows_of(ref, 2 * (2 * unit + p) + n // 3, first, 4) for p in range(2)])

        return self.ninth(tile, step)

    def lhs5(self, unit, step):
        return join([rows_of(self.y3, 2 * unit + p + step // 3, step % 3, 4) for p in range(2)])

    def finish(self, layer, unit, val):
        if layer == 1 and unit in self.keep:
            val = val * self.keep[unit]
        tiles = val.reshape(SUB, TILE, WIDE)
        self.abuf[unit] = tiles
        self.total[0] += jnp.sum(tiles, axis=0)
        self.total[1] += jnp.sum(tiles * tiles, axis=0)

    def conv(self, layer):
        lhs = (self.lhs0, self.lhs1, self.lhs2, self.lhs3, self.lhs4, self.lhs5)[layer]
        steps, ref, count = ((1, self.w1, SUB), (4, self.wr1, 15), (4, self.wd2, SUB), (6, self.wr2, SUB), (5, self.wd3, 4), (9, self.wr3, 4))[layer]
        base = 1 if layer == 1 else 0

        waiting = []

        def drain():
            while waiting:
                units, acc = waiting.pop(0)
                for n, unit in enumerate(units):
                    part = acc[n * UNIT:(n + 1) * UNIT]
                    if layer == 0:
                        self.finish(layer, 2 * unit, part[:, :WIDE])
                        self.finish(layer, 2 * unit + 1, part[:, WIDE:])
                    else:
                        self.finish(layer, unit, part)

        def emit(units, first, last):
            rows = side_by_side([join([lhs(unit, step) for unit in units]) for step in range(first, last)])
            acc = dot(rows, ref[first * WIDE:first * WIDE + rows.shape[1], :])
            drain()
            waiting.append((units, acc))

        def chunk(c):
            emit([base + n for n in range(CHUNK * c, min(CHUNK * (c + 1), count))], 0, steps)

        items = [lambda c=c: chunk(c) for c in range(-(-count // CHUNK))]
        if layer == 1:
            items.append(lambda: emit([0], 2, 4))
            items.append(lambda: emit([TILE], 0, 2))

        def start():
            self.total = [jnp.zeros((TILE, WIDE), F32)] * 2

        def store():
            drain()
            for n in range(2):
                self.sums[n] = self.total[n]

        return [start, *items, store]

    def finalize(self, layer):
        rep = (C1, C2, C3)[layer // 2]
        area = AREAS[layer // 2]
        per_strip = area * rep / (WIDE * SUB)
        count = float(area * rep // SUB)
        bias, gain, offset = self.vecs[layer, 0:1, :], self.vecs[layer, 1:2, :], self.vecs[layer, 2:3, :]
        plain, square = [self.sums[n, :SUB] + self.sums[n, SUB:] for n in range(2)]
        rest = join([plain + per_strip * bias, square + 2.0 * bias * plain + per_strip * bias * bias])
        parts = []
        for _ in range(3):
            parts.append(rest.astype(BF))
            rest = rest - parts[-1].astype(F32)
        grouped = dot(join(parts), self.gmat[layer // 2])
        grouped = grouped[:TILE] + grouped[TILE:2 * TILE] + grouped[2 * TILE:]
        mean = jnp.sum(grouped[:SUB], axis=0, keepdims=True) / count
        power = jnp.sum(grouped[SUB:], axis=0, keepdims=True) / count
        scale = lax.rsqrt(jnp.maximum(power - mean * mean, 0.0) + NORM_EPS) * gain
        self.affine = [jnp.broadcast_to(row, (TILE, WIDE)) for row in (scale, offset + (bias - mean) * scale)]

    def apply(self, block):
        return jnp.maximum(block * self.affine[0] + self.affine[1], 0.0)

    def row0(self, i):
        val = self.apply(self.abuf[self.zero + i])
        self.y1e[i + 1, 0:SUB] = val[..., LOW].astype(BF)
        self.y1o[i + 1, 1:] = val[..., HIGH].astype(BF)
        self.y1o[i + 1, 0] = from_left(val[SUB - 1][:, HIGH], self.strip)
        self.y1e[i + 1, SUB] = from_right(val[0][:, LOW], self.strip)

    def row1(self, i):
        val = self.apply(self.abuf[self.zero + i])
        if i in self.keep:
            val = val * self.keep[i]
        self.z1e[i] = val[..., LOW].astype(BF)
        self.z1o[i, 1:] = val[..., HIGH].astype(BF)
        edge = from_left(val[SUB - 1][:, HIGH], self.strip)
        self.z1o[i, 0] = edge
        if i and i % 2 == 0:
            for q in range(SUB):
                left = val[q - 1][:, HIGH] if q else edge.astype(F32)
                shifted = pltpu.roll(val[q][:, LOW], C1, 1)
                self.z1m[i // 2 - 1, q] = jnp.where(self.lane < C1, left, shifted).astype(BF)

    def row2(self, u):
        val = self.apply(self.abuf[self.zero + u])
        for v, part in enumerate((LOW, HIGH)):
            line = val[..., part]
            self.y2[2 * u + v + 1, 1:SUB + 1] = line.astype(BF)
            self.y2[2 * u + v + 1, 0] = from_left(line[SUB - 1], self.strip)
            self.y2[2 * u + v + 1, SUB + 1] = from_right(line[0], self.strip)

    def row3(self, u):
        val = self.apply(self.abuf[self.zero + u])
        for v, part in enumerate((LOW, HIGH)):
            for q in range(SUB):
                pixel = val[q][:, part]
                if q % 2:
                    self.z2o[2 * u + v + 1, q // 2 + 1] = pixel.astype(BF)
                else:
                    self.z2e[2 * u + v + 1, q // 2] = pixel.astype(BF)
            self.z2o[2 * u + v + 1, 0] = from_left(val[SUB - 1][:, part], self.strip)

    def row4(self, u):
        val = self.apply(self.abuf[self.zero + u])
        for v in range(2):
            line = val[4 * v:4 * v + 4]
            self.y3[2 * u + v + 1, 1:5] = line.astype(BF)
            self.y3[2 * u + v + 1, 0] = side_by_side([from_left(line[3][:, part], self.strip) for part in (LOW, HIGH)])
            self.y3[2 * u + v + 1, 5] = side_by_side([from_right(line[0][:, part], self.strip) for part in (LOW, HIGH)])

    def row5(self, u):
        val = self.apply(self.abuf[self.zero + u])
        for v in range(2):
            for h, part in enumerate((LOW, HIGH)):
                for q in range(4):
                    self.obuf[u, v, h, pl.ds(q, TILE, 4), :] = val[4 * v + q][:, part]
                for w in range(HALVES):
                    self.put(2 * u + w, v, part, self.obuf[u, v, h, 32 * w:32 * w + 32].astype(BF))

    def post(self, layer):
        row, count = ((self.row0, TILE), (self.row1, TILE + 1), (self.row2, SUB), (self.row3, SUB), (self.row4, 4), (self.row5, 4))[layer]
        return [lambda: self.finalize(layer)] + [lambda i=i: row(i) for i in range(count)]


def blend(chunks, rest):
    done = 0
    for n, emit in enumerate(chunks):
        emit()
        goal = len(rest) * (n + 1) // len(chunks)
        for item in rest[done:goal]:
            item()
        done = goal
    for item in rest[done:]:
        item()


def encoder_kernel(image, down1, v1, refine1_in, v2, down2_in, v3, refine2_in, v4, wd3_in, v5, wr3_in, v6, out, inbuf, outbuf, in_send, in_recv, out_send, out_recv, taps,
                   refine1, down2, refine2, wd3, wr3, load_sem, vecs, w1, wr1, wd2, wr2, perm, gmat, af, *buffers):
    group = pl.program_id(0)
    me = 2 * lax.axis_index("h") + lax.axis_index("w")

    def peer(k):
        return lax.rem(me + k, PEERS)

    def device(index):
        return {"h": index // 2, "w": lax.rem(index, 2)}

    def images(index, g):
        return pl.ds(index * PAIR * GROUPS + PAIR * g, PAIR)

    def send_in(g, to, sender):
        return pltpu.make_async_remote_copy(image.at[images(to, g)], inbuf.at[g, sender], in_send, in_recv.at[g], device_id=device(to), device_id_type=MESH)

    def keep_in(g):
        return pltpu.make_async_copy(image.at[images(me, g)], inbuf.at[g, me], in_recv.at[g])

    def send_out(g, to, sender):
        return pltpu.make_async_remote_copy(outbuf.at[g, to], out.at[images(sender, g)], out_send, out_recv, device_id=device(to), device_id_type=MESH)

    def keep_out(g):
        return pltpu.make_async_copy(outbuf.at[g, me], out.at[images(me, g)], out_recv)

    def start_out(g):
        for k in range(1, PEERS):
            send_out(g, peer(k), me).start()
        keep_out(g).start()

    def wait_for(ref, sem):
        pltpu.make_async_copy(ref, ref, sem).wait()

    def wait_in(g):
        wait_for(inbuf.at[g], in_recv.at[g])

    def put_of(e):
        def put(to, v, part, val):
            outbuf[group, to, e, v, :, part] = val

        return put

    zero = (me + group) // (2 * TILE)
    params = (zero, vecs, gmat, w1, wr1, wd2, wr2, wd3, wr3)
    streams = [Stream(params, buffers[e::PAIR], put_of(e)) for e in range(PAIR)]

    def permute(g):
        sides = [join([inbuf[g, HALVES * hh + half, e] for e in range(PAIR) for hh in range(4)]) for half in range(HALVES)]
        af[...] = dot(side_by_side(sides), perm[...]).reshape(af.shape)

    def im2col(e, k):
        rows = []
        for c in range(3):
            block = 24 * e + (k // 2) * 6 + c * 2 + k % 2
            rows += [af[block, :, d * LANES:(d + 1) * LANES] for d in range(PHASES)]
        rows.append(jnp.zeros((SUB, LANES), F32))
        streams[e].bs[k + 1] = join(rows).T.astype(BF).reshape(SUB, TILE, LANES)

    gather = [[lambda e=e, k=k: im2col(e, k) for k in range(SUB)] for e in range(PAIR)]

    @pl.when(group == 0)
    def _():
        pairs = ((refine1_in, refine1), (down2_in, down2), (refine2_in, refine2), (wd3_in, wd3), (wr3_in, wr3))
        loads = [pltpu.make_async_copy(*pair, load_sem.at[n]) for n, pair in enumerate(pairs)]
        for load in loads:
            load.start()
        barrier = pltpu.get_barrier_semaphore()
        for k in range(1, PEERS):
            pl.semaphore_signal(barrier, inc=1, device_id=device(peer(k)), device_id_type=MESH)
        pl.semaphore_wait(barrier, PEERS - 1)

        def begin(g, _):
            keep_in(g).start()
            for k in range(1, PEERS):
                send_in(g, peer(k), me).start()
            return 0

        lax.fori_loop(0, GROUPS, begin, 0)

        expand_first(down1, taps, w1)
        for load in loads:
            load.wait()
        expand_refine1(refine1, wr1)
        expand_rows(down2, wd2, 2, lambda y, x: 4 * x + y if y < 4 else 12 + x)
        expand_rows(refine2, wr2, 1, lambda y, x: 3 * y + x)
        for i, ref in enumerate((v1, v2, v3, v4, v5, v6)):
            vecs[i, 0:3] = side_by_side([ref[...]] * (WIDE // ref.shape[1]))
        row, lane = iota((2 * WIDE, LANES), 0), iota((2 * WIDE, LANES), 1)
        for d in range(PHASES):
            perm[:, d * LANES:(d + 1) * LANES] = one_hot(row == 4 * ((lane % TILE) * SUB + lane // TILE) + d - 1)
        row, lane = iota((WIDE, WIDE), 0), iota((WIDE, WIDE), 1)
        for g, rep in enumerate((C1, C2, C3)):
            gmat[g] = one_hot((row % rep) // (rep // SUB) == (lane % rep) // (rep // SUB))
        for e in range(PAIR):
            bs, _, y1e, y1o, _, _, y2, z2e, z2o, y3 = buffers[e:10 * PAIR:PAIR]
            for ref in (y1e, y1o, y2, y3, z2e, z2o, bs):
                ref[0] = jnp.zeros(ref.shape[1:], BF)
            for ref, last in ((y1e, 17), (y1o, 17), (y2, 17), (y3, 9)):
                ref[last] = jnp.zeros(ref.shape[1:], BF)

        wait_in(0)
        permute(0)
        for item in (*gather[0], *gather[1], *streams[0].conv(0)):
            item()

    @pl.when(group > 0)
    def _():
        start_out(group - 1)

    first, second = streams
    following = lax.rem(group + 1, GROUPS)
    for layer in range(6):
        extra = gather[0] + gather[1] if layer == 5 else []
        blend(second.conv(layer), first.post(layer) + extra)
        if layer == 4:
            pl.when(group < GROUPS - 1)(lambda: wait_in(following))
        extra = [lambda: permute(following)] if layer == 4 else []
        blend(extra + first.conv(layer + 1 if layer < 5 else 0), second.post(layer))

    @pl.when(group == GROUPS - 1)
    def _():
        others = pl.ds(0, PAIR * GROUPS * (PEERS - 1))
        wait_for(image.at[others], in_send)
        start_out(group)
        wait_for(out.at[others], out_send)
        wait_for(out, out_recv)


def solution(mesh):
    act_spec = P("batch", "h", "w")
    sem = pltpu.SemaphoreType.DMA
    scratch = [
        ((GROUPS, PEERS, PAIR, PIECE_ROWS, PIECE_COLS), BF), ((GROUPS, PEERS, PAIR, 2, 32, WIDE), BF), sem, sem((GROUPS,)), sem, sem, ((32, C1), F32),
        ((3, 3, C1, C1), BF), ((3, 3, C1, C2), BF), ((3, 3, C2, C2), BF), ((1152, WIDE), BF), ((2304, WIDE), BF), pltpu.SemaphoreType.DMA((5,)),
        ((8, 8, WIDE), F32), ((WIDE, 512), BF), ((1024, WIDE), BF), ((1024, WIDE), BF), ((1536, WIDE), BF),
        ((512, 640), BF), ((3, WIDE, WIDE), BF), ((48, SUB, 640), F32),
    ]
    for shape, dtype in (
        ((9, SUB, TILE, LANES), BF), ((17, SUB, TILE, WIDE), F32), ((20, 9, TILE, LANES), BF), ((20, 9, TILE, LANES), BF), ((17, 8, TILE, LANES), BF),
        ((20, 9, TILE, LANES), BF), ((18, 10, TILE, LANES), BF), ((17, 4, TILE, LANES), BF), ((20, 5, TILE, LANES), BF), ((10, 6, TILE, WIDE), BF),
        ((4, 2, 2, 64, LANES), F32), ((2, TILE, WIDE), F32), ((8, SUB, TILE, LANES), BF),
    ):
        scratch += [(shape, dtype)] * PAIR

    def local_forward(tile, *params):
        planes = tile.transpose(0, 3, 1, 2).reshape(-1, PIECE_ROWS, PIECE_COLS)
        params = list(params)
        params[8], params[10] = params[8].reshape(-1, WIDE), params[10].reshape(-1, WIDE)
        result = pl.pallas_call(
            encoder_kernel,
            grid=(GROUPS,),
            out_shape=jax.ShapeDtypeStruct((128, 2, 32, WIDE), BF),
            in_specs=[pl.BlockSpec(memory_space=pltpu.HBM if n in (0, 3, 5, 7, 9, 11) else pltpu.VMEM) for n in range(13)],
            out_specs=pl.BlockSpec(memory_space=pl.ANY),
            scratch_shapes=[pltpu.VMEM(*entry) if isinstance(entry, tuple) else entry for entry in scratch],
            compiler_params=pltpu.CompilerParams(vmem_limit_bytes=60 * 1024 * 1024, collective_id=0, has_side_effects=True),
            name="encoder",
        )(planes, *params)
        return jnp.maximum(result, 0)

    return jax.shard_map(local_forward, mesh=mesh, in_specs=(act_spec,) + (P(),) * 12, out_specs=act_spec, check_vma=False)
```
